32 devices in a mesh: gx: 4 (over z), gy: 4 (over y, x), gz: 2 (over core).
Axes of the slice: x: 2, y: 2, z: 4, core: 2. Of those that a mesh axis runs over, the one named last changes fastest.
Arguments:
- potential: float32 [16, 96, 512], P('gz', 'gx', 'gy'), may hold values from -6 to 6
- tissue_mask: int32 [16, 96, 512], P('gz', 'gx', 'gy'), may hold values from 0 to 2, as said below
- layer_index: int32 [16], P('gz'), may hold values from 0 to 15
- source: float32 [16, 96, 512], P('gz', 'gx', 'gy'), may hold values from -6 to 6
Outputs:
- phi_e: float32 [16, 96, 512], P('gz', 'gx', 'gy')
- residual: float32 [16, 96, 512], P('gz', 'gx', 'gy')
The draws below stay inside these ranges and needn't reach their ends.
Inputs may be any that keep to these rules, and one draw needn't show every extreme that they name: `tissue_mask`: 0 marks cells outside every medium, 1 bath, 2 tissue.
All inputs are finite; a program needn't handle non-finite values.
Results may differ from the reference program's by a relative error of at most 0.0003.
Values sent between devices are 32-bit elements; how exact they have to be, the bound alone decides.
No kernel may reach another device: no remote copies, remote signals or barrier semaphores. Data moves between devices by JAX's collectives and lax.ppermute only.
A program may use at most 128 MiB of HBM per device.

```python
import math
import jax
import jax.numpy as jnp

ITERS = 8
LAYERS = 16
NZ = 16
NX = 96
NY = 512


def cell_axes():
    plane_z = jnp.arange(NZ, dtype=jnp.float32)[:, None, None] + 0.5
    row_x = jnp.arange(NX, dtype=jnp.float32)[None, :, None] + 0.5
    column_y = jnp.arange(NY, dtype=jnp.float32)[None, None, :] + 0.5
    return (plane_z, row_x, column_y)


def draw_tissue_mask(key, part):
    centre_key = jax.random.fold_in(key, 101)
    radius_key = jax.random.fold_in(key, 103)
    jitter_key = jax.random.fold_in(key, 107)
    shift = jax.random.randint(centre_key, (3,), -8, 9)
    centre_z = NZ // 2 + shift[0] * NZ // 64
    centre_x = NX // 2 + shift[1] * NX // 64
    centre_y = NY // 2 + shift[2] * NY // 64
    plane_z = jnp.arange(NZ, dtype=jnp.int32)[:, None, None]
    row_x = jnp.arange(NX, dtype=jnp.int32)[None, :, None]
    column_y = jnp.arange(NY, dtype=jnp.int32)[None, None, :]
    scaled_z = 128 * (plane_z - centre_z) // NZ
    scaled_x = 128 * (row_x - centre_x) // NX
    scaled_y = 128 * (column_y - centre_y) // NY
    reach = scaled_z * scaled_z + scaled_x * scaled_x + scaled_y * scaled_y
    reach = reach + jax.random.randint(jitter_key, (NZ, NX, NY), -150, 151)
    inner_key, outer_key, bath_key = jax.random.split(radius_key, 3)
    inner_edge = jax.random.randint(inner_key, (), 600, 1001)
    outer_edge = jax.random.randint(outer_key, (), 1900, 2501)
    bath_edge = jax.random.randint(bath_key, (), 3200, 4201)
    labels = jnp.where(reach < inner_edge, 1, jnp.where(reach < outer_edge, 2, jnp.where(reach < bath_edge, 1, 0)))
    return labels.astype(jnp.int32)


def draw_potential(key, part):
    normal_key = jax.random.fold_in(key, 201)
    anchor_key = jax.random.fold_in(key, 203)
    shape_key = jax.random.fold_in(key, 207)
    noise_key = jax.random.fold_in(key, 211)
    plane_z, row_x, column_y = cell_axes()
    sizes = jnp.array([NZ, NX, NY], jnp.float32)
    anchor = jax.random.uniform(anchor_key, (3,), jnp.float32, 0.3, 0.7) * sizes
    amp_key, width_key = jax.random.split(shape_key, 2)
    width = jax.random.uniform(width_key, (), jnp.float32, 2.0, 5.0)
    direction = jax.random.normal(normal_key, (3,), jnp.float32)
    direction = direction / jnp.sqrt(jnp.sum(direction * direction) + 1e-06)
    signed = direction[0] * (plane_z - anchor[0]) + direction[1] * (row_x - anchor[1]) + direction[2] * (column_y - anchor[2])
    amplitude = jax.random.uniform(amp_key, (), jnp.float32, 2.0, 4.0)
    noise = jnp.clip(0.5 * jax.random.normal(noise_key, (NZ, NX, NY), jnp.float32), -2.0, 2.0)
    return (amplitude * jnp.tanh(signed / width) + noise).astype(jnp.float32)


def draw_source(key, part):
    sign_key = jax.random.fold_in(key, 301)
    level_key = jax.random.fold_in(key, 303)
    mode_key = jax.random.fold_in(key, 307)
    weight_key = jax.random.fold_in(key, 311)
    noise_key = jax.random.fold_in(key, 313)
    plane_z, row_x, column_y = cell_axes()
    sign = jnp.where(jax.random.bernoulli(sign_key), 1.0, -1.0).astype(jnp.float32)
    orders = jax.random.randint(mode_key, (3, 3), 0, 3).astype(jnp.float32)
    level = jax.random.uniform(level_key, (), jnp.float32, 0.5, 1.0)
    weights = jax.random.uniform(weight_key, (3,), jnp.float32, -0.5, 0.5)
    noise = jnp.clip(jax.random.normal(noise_key, (NZ, NX, NY), jnp.float32), -3.0, 3.0)
    smooth = jnp.zeros((NZ, NX, NY), jnp.float32)
    for mode in range(3):
        wave = jnp.cos(math.pi * orders[mode, 0] * plane_z / NZ) * jnp.cos(math.pi * orders[mode, 1] * row_x / NX)
        wave = wave * jnp.cos(math.pi * orders[mode, 2] * column_y / NY)
        smooth = smooth + weights[mode] * wave
    return (sign * level + smooth + noise).astype(jnp.float32)


def with_ends(result, key, smallest, largest):
    place = [jax.random.randint(jax.random.fold_in(key, axis), (), 0, length) for axis, length in enumerate(result.shape)]
    main_axis = result.shape.index(max(result.shape))
    next_to = place[:main_axis] + [(place[main_axis] + 1) % result.shape[main_axis]] + place[main_axis + 1:]
    return result.at[tuple(place)].set(smallest).at[tuple(next_to)].set(largest)


def setup_inputs(seed: int = 0) -> dict:
    arg_keys = jax.random.split(jax.random.key(seed), 5)
    potential = draw_potential(jax.random.fold_in(arg_keys[4], 71), 0)
    tissue_mask = draw_tissue_mask(jax.random.fold_in(arg_keys[4], 71), 0)
    layer_index = with_ends(jax.random.randint(arg_keys[2], (NZ,), 0, LAYERS), jax.random.fold_in(arg_keys[2], 1), 0, LAYERS - 1).astype(jnp.int32)
    source = draw_source(jax.random.fold_in(arg_keys[4], 71), 0)
    return dict(potential=potential, tissue_mask=tissue_mask, layer_index=layer_index, source=source)


OFFSETS = [(0, 1, 0), (0, 0, 1), (1, 0, 0), (0, 1, 1), (0, 1, -1), (1, 1, 0), (-1, 1, 0), (1, 0, 1), (-1, 0, 1)]
bulk_long = 7.99
bulk_trans = 2.55
intra_long = 1.74
intra_trans = 0.19
bath_sigma = 5.0


def tensor_table(layers, longitudinal, transverse):
    depth = jnp.arange(layers, dtype=jnp.float32) / (layers - 1)
    helix = (math.pi / 3.0) * (1.0 - 2.0 * depth)
    tilted = 0.35 * jnp.cos(math.pi * depth)
    fiber_x = jnp.cos(tilted) * jnp.cos(helix)
    fiber_y = jnp.cos(tilted) * jnp.sin(helix)
    fiber_z = jnp.sin(tilted)
    spread = longitudinal - transverse
    s_xx = transverse + spread * fiber_x * fiber_x
    s_yy = transverse + spread * fiber_y * fiber_y
    s_zz = transverse + spread * fiber_z * fiber_z
    s_xy = spread * fiber_x * fiber_y
    s_xz = spread * fiber_x * fiber_z
    s_yz = spread * fiber_y * fiber_z
    columns = [s_xx - jnp.abs(s_xy) - jnp.abs(s_xz), s_yy - jnp.abs(s_xy) - jnp.abs(s_yz),
               s_zz - jnp.abs(s_xz) - jnp.abs(s_yz), jnp.maximum(s_xy, 0.0), jnp.maximum(-s_xy, 0.0),
               jnp.maximum(s_xz, 0.0), jnp.maximum(-s_xz, 0.0), jnp.maximum(s_yz, 0.0), jnp.maximum(-s_yz, 0.0)]
    return jnp.stack(columns, axis=1).astype(jnp.float32)


def window(array, offset, extent):
    return array[1 + offset[0]:1 + offset[0] + extent[0], 1 + offset[1]:1 + offset[1] + extent[1],
                 1 + offset[2]:1 + offset[2] + extent[2]]


def cell_weight(planes, column, tissue_pad, bath_pad):
    weight = tissue_pad * planes[:, column][:, None, None]
    if bath_pad is not None and column < 3:
        weight = weight + bath_sigma * bath_pad
    return weight


def edge_pair(weight, medium_pad, offset, extent):
    backward = (-offset[0], -offset[1], -offset[2])
    centre = window(medium_pad, (0, 0, 0), extent)
    own_weight = window(weight, (0, 0, 0), extent)
    forward_edge = centre * window(medium_pad, offset, extent) * (0.5 * (own_weight + window(weight, offset, extent)))
    backward_edge = centre * window(medium_pad, backward, extent) * (0.5 * (own_weight + window(weight, backward, extent)))
    return forward_edge, backward_edge


def operate(field, planes, tissue_pad, bath_pad, medium_pad):
    extent = field.shape
    field_pad = jnp.pad(field, 1)
    summed = jnp.zeros(extent, jnp.float32)
    for column, offset in enumerate(OFFSETS):
        backward = (-offset[0], -offset[1], -offset[2])
        weight = cell_weight(planes, column, tissue_pad, bath_pad)
        forward_edge, backward_edge = edge_pair(weight, medium_pad, offset, extent)
        summed = summed + forward_edge * (field - window(field_pad, offset, extent)) + backward_edge * (field - window(field_pad, backward, extent))
    return summed


def reference(potential, tissue_mask, layer_index, source):
    extent = tissue_mask.shape
    mask_pad = jnp.pad(tissue_mask, 1)
    layer_pad = jnp.pad(layer_index, 1)
    tissue_pad = (mask_pad == 2).astype(jnp.float32)
    bath_pad = (mask_pad == 1).astype(jnp.float32)
    inside_pad = (mask_pad > 0).astype(jnp.float32)
    inside = window(inside_pad, (0, 0, 0), extent)
    bulk_planes = tensor_table(LAYERS, bulk_long, bulk_trans)[layer_pad]
    intra_planes = tensor_table(LAYERS, intra_long, intra_trans)[layer_pad]
    diagonal = jnp.zeros(extent, jnp.float32)
    for column, offset in enumerate(OFFSETS):
        weight = cell_weight(bulk_planes, column, tissue_pad, bath_pad)
        forward_edge, backward_edge = edge_pair(weight, inside_pad, offset, extent)
        diagonal = diagonal + forward_edge + backward_edge
    jacobi = inside / jnp.maximum(diagonal, 1.0)
    rhs = -operate(potential, intra_planes, tissue_pad, None, tissue_pad) + inside * source
    count = jnp.sum(inside)
    residual = rhs - inside * (jnp.sum(rhs) / count)

    def precondition(current):
        scaled = jacobi * current
        return scaled - inside * (jnp.sum(scaled) / count)

    solution = jnp.zeros(extent, jnp.float32)
    precond = precondition(residual)
    direction = precond
    rz_now = jnp.sum(residual * precond)
    for step in range(ITERS):
        image = operate(direction, bulk_planes, tissue_pad, bath_pad, inside_pad)
        alpha = rz_now / jnp.sum(direction * image)
        solution = solution + alpha * direction
        residual = residual - alpha * image
        if step + 1 < ITERS:
            precond = precondition(residual)
            rz_next = jnp.sum(residual * precond)
            direction = precond + (rz_next / rz_now) * direction
            rz_now = rz_next
    return solution, residual
```

```python
import functools
import math

import jax
import jax.numpy as jnp
import numpy as np
from jax import lax
from jax.experimental import pallas as pl
from jax.experimental.pallas import tpu as pltpu
from jax.sharding import PartitionSpec as P

ITERS = 8
LAYERS = 16
HALO = ITERS + 1
LANES = 128
SLOT = 16
TOP = 16
VECS = ITERS + 1
SUMS = VECS * VECS

OFFSETS = [
    (0, 1, 0),
    (0, 0, 1),
    (1, 0, 0),
    (0, 1, 1),
    (0, 1, -1),
    (1, 1, 0),
    (-1, 1, 0),
    (1, 0, 1),
    (-1, 0, 1),
]
bulk_long = 7.99
bulk_trans = 2.55
intra_long = 1.74
intra_trans = 0.19
bath_sigma = 5.0

VMEM = pl.BlockSpec(memory_space=pltpu.VMEM)
SMEM = pl.BlockSpec(memory_space=pltpu.SMEM)


def tensor_table(layers, longitudinal, transverse):
    depth = np.arange(layers, dtype=np.float64) / (layers - 1)
    helix = math.pi / 3.0 * (1.0 - 2.0 * depth)
    tilted = 0.35 * np.cos(math.pi * depth)
    fiber_x = np.cos(tilted) * np.cos(helix)
    fiber_y = np.cos(tilted) * np.sin(helix)
    fiber_z = np.sin(tilted)
    spread = longitudinal - transverse
    s_xx = transverse + spread * fiber_x * fiber_x
    s_yy = transverse + spread * fiber_y * fiber_y
    s_zz = transverse + spread * fiber_z * fiber_z
    s_xy = spread * fiber_x * fiber_y
    s_xz = spread * fiber_x * fiber_z
    s_yz = spread * fiber_y * fiber_z
    columns = [
        s_xx - np.abs(s_xy) - np.abs(s_xz),
        s_yy - np.abs(s_xy) - np.abs(s_yz),
        s_zz - np.abs(s_xz) - np.abs(s_yz),
        np.maximum(s_xy, 0.0),
        np.maximum(-s_xy, 0.0),
        np.maximum(s_xz, 0.0),
        np.maximum(-s_xz, 0.0),
        np.maximum(s_yz, 0.0),
        np.maximum(-s_yz, 0.0),
    ]
    return np.stack(columns, axis=1).astype(np.float32)


def lane_iota(shape):
    return lax.broadcasted_iota(jnp.int32, shape, len(shape) - 1)


def roll(value, shift, axis=-1):
    axis = axis % value.ndim
    shift = shift % value.shape[axis]
    return value if shift == 0 else pltpu.roll(value, shift, axis)


def pack_y(geometry, offs, *refs):
    pieces, own_count, planes, rows, full = geometry
    piece_refs = refs[: len(pieces)]
    joined, left, right, sums = refs[len(pieces) :]
    for number, length in enumerate(pieces):
        for plane in range(length):
            at = offs[number] + plane
            for field in range(3):
                joined[field, at] = piece_refs[number][field, plane]
    lane = lane_iota((rows, LANES))
    count = jnp.zeros((rows, LANES), jnp.float32)
    total = jnp.zeros((rows, LANES), jnp.float32)
    for number, length in enumerate(pieces):
        if full or number == own_count:
            for plane in range(length):
                inside = jnp.minimum(piece_refs[number][2, plane], 1.0)
                count = count + inside
                total = total + inside * piece_refs[number][1, plane]
    sums[...] = jnp.zeros((8, LANES), jnp.float32)
    sums[0:1] = jnp.sum(count, axis=0, keepdims=True)
    sums[1:2] = jnp.sum(total, axis=0, keepdims=True)
    groups = -(-planes // 8)
    for field in range(3):
        for group in range(groups):
            to_left = jnp.zeros((rows, LANES), jnp.float32)
            to_right = jnp.zeros((rows, LANES), jnp.float32)
            for slot in range(min(8, planes - 8 * group)):
                value = joined[field, 8 * group + slot]
                here = (lane >= SLOT * slot) & (lane < SLOT * (slot + 1))
                to_left = jnp.where(here, roll(value, SLOT * slot), to_left)
                to_right = jnp.where(here, roll(value, SLOT * (slot + 1)), to_right)
            base = (field * groups + group) * rows
            left[base : base + rows] = to_left
            right[base : base + rows] = to_right
    last = 3 * groups * rows
    left[last : last + 8] = sums[...]
    right[last : last + 8] = sums[...]


def pack_x(geometry, joined, from_left, from_right, *refs):
    planes, rows, others = geometry
    other_refs = refs[:others]
    upper, lower, sums = refs[others:]
    groups = -(-planes // 8)
    last = 3 * groups * rows
    total = from_left[last : last + 8] + from_right[last : last + 8]
    for ref in other_refs:
        total = total + ref[...]
    sums[...] = total
    row = 0
    for field in range(3):
        for plane in range(planes):
            upper[row : row + HALO] = joined[field, plane, 0:HALO]
            lower[row : row + HALO] = joined[field, plane, rows - HALO : rows]
            row += HALO
    for strip in (from_left, from_right):
        for block in range(3 * groups):
            base = block * rows
            upper[row : row + HALO] = strip[base : base + HALO]
            lower[row : row + HALO] = strip[base + rows - HALO : base + rows]
            row += HALO
    row = -(-row // 8) * 8
    upper[row : row + 8] = total
    lower[row : row + 8] = total


def x_rows(planes):
    groups = -(-planes // 8)
    return -(-HALO * 3 * (planes + 2 * groups) // 8) * 8


def krylov(geometry, info, offs, table, *refs):
    pieces, planes, own_planes, rows, others = geometry
    layer_refs = refs[: len(pieces)]
    refs = refs[len(pieces) :]
    joined, from_left, from_right, from_upper, from_lower, total_in = refs[:6]
    refs = refs[6:]
    gram, basis, metric, extra = refs[:4]
    layer, pot, med, edge, edge_r, vec, vec_l, vec_r, jac, kap, acc, rowsum = refs[4:]
    groups = -(-planes // 8)
    tiles = 2
    high = TOP + rows + 16
    inner = (rows + 16) // 8
    lane = lane_iota((8, LANES))
    has_left, has_right, has_upper, has_lower, first = (info[i] for i in range(5))

    layer[0] = 0
    layer[planes + 1] = 0
    for number, length in enumerate(pieces):
        for plane in range(length):
            layer[offs[number] + plane + 1] = layer_refs[number][plane]

    count = jnp.sum(total_in[0:1], axis=1, keepdims=True)
    mean = jnp.sum(total_in[1:2], axis=1, keepdims=True) / count

    zero = jnp.zeros((8, LANES), jnp.float32)
    as_float = lambda flag: flag.astype(jnp.float32)
    keep_left = as_float(has_left)
    keep_right = as_float(has_right)
    keep_upper = as_float(has_upper)
    keep_lower = as_float(has_lower)
    for buffer in (pot, med):
        for copy in range(3):
            for tile in range(tiles):
                for plane in (0, planes + 1):
                    for at in range(0, high, 8):
                        buffer[copy, tile, plane, at : at + 8] = zero

    def place(buffer, tile, plane, at, value):
        size = value.shape[0]
        buffer[0, tile, plane, at : at + size] = value
        buffer[1, tile, plane, at : at + size] = roll(value, LANES - 1)
        buffer[2, tile, plane, at : at + size] = roll(value, 1)

    half = 3 * planes * HALO
    for slot_group in range(groups):
        for slot in range(min(8, planes - 8 * slot_group)):
            z = 8 * slot_group + slot
            for kind, field in enumerate((0, 2)):
                buffer = (pot, med)[kind]
                block = field * groups + slot_group

                def split(own, strip_l, strip_r, keep):
                    size = own.shape[0]
                    ln = lane_iota((size, LANES))
                    a = roll(strip_l, LANES - SLOT * slot)
                    b = roll(strip_r, LANES - SLOT * (slot + 1))
                    if kind == 1:
                        a, b = a * keep_left, b * keep_right
                    low = jnp.where(ln < SLOT, a, roll(own, SLOT))
                    up = jnp.where(ln >= LANES - SLOT, b, roll(own, LANES - SLOT))
                    if kind == 1 and keep is not None:
                        low, up = low * keep, up * keep
                    return low, up

                own = joined[field, z]
                strip_l = from_left[block * rows : (block + 1) * rows]
                strip_r = from_right[block * rows : (block + 1) * rows]
                for tile, value in enumerate(split(own, strip_l, strip_r, None)):
                    place(buffer, tile, z + 1, TOP, value)
                for strip, keep, at in (
                    (from_upper, keep_upper, TOP - HALO),
                    (from_lower, keep_lower, TOP + rows),
                ):
                    r0 = (field * planes + z) * HALO
                    r1 = half + block * HALO
                    r2 = half + (3 * groups + block) * HALO
                    values = split(
                        strip[r0 : r0 + HALO], strip[r1 : r1 + HALO], strip[r2 : r2 + HALO], keep
                    )
                    for tile, value in enumerate(values):
                        for copy in range(3):
                            edge_at = 0 if at < TOP else high - 8
                            buffer[copy, tile, z + 1, edge_at : edge_at + 8] = zero
                        place(buffer, tile, z + 1, at, value)

    for slot_group in range(groups):
        for slot in range(min(8, planes - 8 * slot_group)):
            z = 8 * slot_group + slot
            block = groups + slot_group

            def spread(own, strip_l, strip_r):
                ln = lane_iota(own.shape)
                a = roll(strip_l, LANES - SLOT * slot)
                b = roll(strip_r, LANES - SLOT * (slot + 1))
                low = jnp.where(ln < SLOT, a, roll(own, SLOT))
                up = jnp.where(ln >= LANES - SLOT, b, roll(own, LANES - SLOT))
                return low, up

            own = joined[1, z]
            strip_l = from_left[block * rows : (block + 1) * rows]
            strip_r = from_right[block * rows : (block + 1) * rows]
            for tile, value in enumerate(spread(own, strip_l, strip_r)):
                vec[2, tile, z + 1, TOP : TOP + rows] = value
            for strip, at, skip in ((from_upper, TOP - 8, 1), (from_lower, TOP + rows, 0)):
                r0 = (planes + z) * HALO + skip
                r1 = half + block * HALO + skip
                r2 = half + (3 * groups + block) * HALO + skip
                values = spread(strip[r0 : r0 + 8], strip[r1 : r1 + 8], strip[r2 : r2 + 8])
                for tile, value in enumerate(values):
                    vec[2, tile, z + 1, at : at + 8] = value

    shifted = {0: 0, 1: 1, -1: 2}
    rolled = [column for column, offset in enumerate(OFFSETS) if offset[2]]

    for column, (dz, _, dy) in enumerate(OFFSETS):
        if dz:
            plane = 0 if dz > 0 else planes + 1
            for tile in range(tiles):
                for at in range(0, 8 * (inner + 1), 8):
                    if dy:
                        edge_r[rolled.index(column), tile, plane, at : at + 8] = zero
                    else:
                        edge[column, tile, plane, at : at + 8] = zero

    def edges_of(z, carry):
        here = layer[z + 1] * 18
        for tile in range(tiles):
            for block in range(inner + 1):
                at = 8 * block
                m = med[0, tile, z + 1, at : at + 8]
                inside = jnp.minimum(m, 1.0)
                tissue = jnp.maximum(m - 1.0, 0.0)
                bath = (inside - tissue) * (0.5 * bath_sigma)
                for column, (dz, dx, dy) in enumerate(OFFSETS):
                    there = layer[z + 1 + dz] * 18
                    if block == 0 and dx < 0:
                        raise ValueError("row order")
                    n = med[shifted[dy], tile, z + 1 + dz, at + dx : at + dx + 8]
                    n_in = jnp.minimum(n, 1.0)
                    n_ti = jnp.maximum(n - 1.0, 0.0)
                    weight = tissue * table[here + column] + n_ti * table[there + column]
                    if column < 3:
                        weight = weight + (bath + (n_in - n_ti) * (0.5 * bath_sigma))
                    weight = (inside * n_in) * weight
                    edge[column, tile, z + 1, at : at + 8] = weight
                    if dy:
                        edge_r[rolled.index(column), tile, z + 1, at : at + 8] = roll(weight, dy)
        return carry

    lax.fori_loop(0, planes, edges_of, 0)

    for copy in range(3):
        for tile in range(tiles):
            for plane in (0, planes + 1):
                for at in range(0, high, 8):
                    vec[copy, tile, plane, at : at + 8] = zero
                    if copy < 2:
                        vec_l[copy, tile, plane, at : at + 8] = zero
                        vec_r[copy, tile, plane, at : at + 8] = zero
            for plane in range(1, planes + 1):
                for at in (0, high - 8):
                    vec[copy, tile, plane, at : at + 8] = zero
                    if copy < 2:
                        vec_l[copy, tile, plane, at : at + 8] = zero
                        vec_r[copy, tile, plane, at : at + 8] = zero

    def backward(column, tile, z, at):
        dz, dx, dy = OFFSETS[column]
        if dy:
            return edge_r[rolled.index(column), tile, z + 1 - dz, at - dx : at - dx + 8]
        return edge[column, tile, z + 1 - dz, at - dx : at - dx + 8]

    def start_of(z, carry):
        here = layer[z + 1] * 18 + 9
        for tile in range(tiles):
            for block in range(inner):
                at = 8 + 8 * block
                m = med[0, tile, z + 1, at : at + 8]
                inside = jnp.minimum(m, 1.0)
                tissue = jnp.maximum(m - 1.0, 0.0)
                value = pot[0, tile, z + 1, at : at + 8]
                diagonal = zero
                flow = zero
                for column, (dz, dx, dy) in enumerate(OFFSETS):
                    forward_edge = edge[column, tile, z + 1, at : at + 8]
                    diagonal = diagonal + forward_edge + backward(column, tile, z, at)
                    for sign in (1, -1):
                        there = layer[z + 1 + sign * dz] * 18 + 9
                        scale = table[here + column] + table[there + column]
                        r = at + sign * dx
                        n = med[shifted[sign * dy], tile, z + 1 + sign * dz, r : r + 8]
                        v = pot[shifted[sign * dy], tile, z + 1 + sign * dz, r : r + 8]
                        flow = flow + (jnp.maximum(n - 1.0, 0.0) * scale) * (v - value)
                source = vec[2, tile, z + 1, at : at + 8]
                residual = tissue * flow + inside * source - inside * mean
                size = jnp.maximum(diagonal, 1.0)
                scale = inside / size
                jac[tile, z + 1, at : at + 8] = scale
                kap[tile, z + 1, at : at + 8] = jnp.where(
                    diagonal >= 1.0, 0.0, inside - scale * diagonal
                )
                first_vec = scale * residual
                vec[0, tile, z + 1, at : at + 8] = first_vec
                vec_l[0, tile, z + 1, at : at + 8] = roll(first_vec, LANES - 1)
                vec_r[0, tile, z + 1, at : at + 8] = roll(first_vec, 1)
                vec[1, tile, z + 1, at : at + 8] = inside * size
                vec_l[1, tile, z + 1, at : at + 8] = residual
        return carry

    lax.fori_loop(0, planes, start_of, 0)

    def merged(buffer, plane, at):
        low = roll(buffer[0, plane, at : at + 8], LANES - SLOT)
        up = roll(buffer[1, plane, at : at + 8], SLOT)
        return jnp.where(lane < LANES // 2, low, up)

    def own_of(z, carry):
        for block in range(rows // 8):
            at = TOP + 8 * block
            out = 8 * block
            metric[z, out : out + 8] = merged(vec.at[1], first + z + 1, at)
            extra[z, out : out + 8] = merged(vec_l.at[1], first + z + 1, at)
            basis[0, z, out : out + 8] = merged(vec.at[0], first + z + 1, at)
        return carry

    lax.fori_loop(0, own_planes, own_of, 0)

    for step in range(ITERS):
        now, later, before = step % 3, (step + 1) % 3, (step + 2) % 3
        side, side_next = step % 2, (step + 1) % 2
        reach = ITERS - 1 - step
        sources = {0: vec.at[now], 1: vec_l.at[side], -1: vec_r.at[side]}

        def apply(z, carry):
            for tile in range(tiles):
                for block in range(inner):
                    at = 8 + 8 * block
                    total = zero
                    for column, (dz, dx, dy) in enumerate(OFFSETS):
                        total = total + edge[column, tile, z + 1, at : at + 8] * sources[dy][
                            tile, z + 1 + dz, at + dx : at + dx + 8
                        ]
                        total = total + backward(column, tile, z, at) * sources[-dy][
                            tile, z + 1 - dz, at - dx : at - dx + 8
                        ]
                    value = (
                        jac[tile, z + 1, at : at + 8] * total
                        + kap[tile, z + 1, at : at + 8] * sources[0][tile, z + 1, at : at + 8]
                    )
                    if step:
                        value = 2.0 * value - vec[before, tile, z + 1, at : at + 8]
                    vec[later, tile, z + 1, at : at + 8] = value
                    if step + 1 < ITERS:
                        vec_l[side_next, tile, z + 1, at : at + 8] = roll(value, LANES - 1)
                        vec_r[side_next, tile, z + 1, at : at + 8] = roll(value, 1)
            return carry

        low = jnp.maximum(first - reach, 0)
        up = jnp.minimum(first + own_planes + reach, planes)
        lax.fori_loop(low, up, apply, 0)

        def keep(z, carry):
            for block in range(rows // 8):
                at = TOP + 8 * block
                out = 8 * block
                basis[step + 1, z, out : out + 8] = merged(vec.at[later], first + z + 1, at)
            return carry

        lax.fori_loop(0, own_planes, keep, 0)

    acc[...] = jnp.zeros(acc.shape, jnp.float32)
    pairs = [(i, j) for i in range(VECS) for j in range(i, VECS)]
    split_at = 26
    for part in (pairs[:split_at], pairs[split_at:]):
        plain = part is not pairs[:split_at] and part[-1] == pairs[-1]

        def gather(z, carry):
            carry = list(carry)
            for block in range(rows // 8):
                out = 8 * block
                weight = metric[z, out : out + 8]
                loaded = {}
                for i, j in part:
                    for index in (i, j):
                        if index not in loaded:
                            loaded[index] = basis[index, z, out : out + 8]
                scaled = {i: loaded[i] * weight for i in {i for i, _ in part}}
                for number, (i, j) in enumerate(part):
                    carry[number] = carry[number] + scaled[i] * loaded[j]
            return tuple(carry)

        done = lax.fori_loop(0, own_planes, gather, tuple(zero for _ in part))
        for (i, j), value in zip(part, done):
            value = jnp.sum(value, axis=0, keepdims=True)
            rowsum[VECS * i + j : VECS * i + j + 1] = value
            if i != j:
                rowsum[VECS * j + i : VECS * j + i + 1] = value

    def plain_sums(z, carry):
        carry = list(carry)
        for block in range(rows // 8):
            out = 8 * block
            for index in range(ITERS):
                carry[index] = carry[index] + basis[index, z, out : out + 8]
            carry[ITERS] = carry[ITERS] + extra[z, out : out + 8]
        return tuple(carry)

    done = lax.fori_loop(0, own_planes, plain_sums, tuple(zero for _ in range(ITERS + 1)))
    for index, value in enumerate(done):
        rowsum[SUMS + index : SUMS + index + 1] = jnp.sum(value, axis=0, keepdims=True)
    for index in range(SUMS + ITERS + 1, rowsum.shape[0]):
        rowsum[index : index + 1] = jnp.zeros((1, LANES), jnp.float32)
    gram[...] = lax.dot_general(
        jnp.ones((8, LANES), jnp.float32),
        rowsum[...],
        (((1,), (1,)), ((), ())),
        precision=lax.Precision.HIGHEST,
        preferred_element_type=jnp.float32,
    )


def finish(geometry, gathered, total_in, basis, metric, solution_ref, residual_ref, flag):
    own_planes, rows = geometry
    total = jnp.sum(gathered[...], axis=0, keepdims=True)
    count = jnp.sum(total_in[0:1], axis=1, keepdims=True)
    lane = lane_iota((16, LANES))
    sub = lax.broadcasted_iota(jnp.int32, (16, LANES), 0)
    matrix = jnp.zeros((16, LANES), jnp.float32)
    for i in range(VECS):
        line = roll(total, LANES - VECS * i)
        matrix = jnp.where(sub == i, jnp.broadcast_to(line, (16, LANES)), matrix)
    matrix = jnp.where(lane < VECS, matrix, 0.0)
    reflected = jnp.where(lane == 0, roll(matrix, LANES - 1), roll(matrix, 1))
    square = matrix - 0.5 * (roll(matrix, LANES - 1) + reflected)
    system = jnp.where(lane < ITERS, square, 0.0)
    system = jnp.where(lane == ITERS, roll(matrix, ITERS), system)[0:8]
    lane8 = lane[0:8]
    sub8 = sub[0:8]
    for k in range(ITERS):
        line = system[k : k + 1]
        pivot = jnp.sum(jnp.where(lane8[0:1] == k, line, 0.0), axis=1, keepdims=True)
        line = line / pivot
        column = jnp.sum(jnp.where(lane8 == k, system, 0.0), axis=1, keepdims=True)
        line8 = jnp.broadcast_to(line, (8, LANES))
        system = jnp.where(sub8 == k, line8, system - column * line8)
    answer = jnp.sum(jnp.where(lane8 == ITERS, system, 0.0), axis=1, keepdims=True)
    coef = [answer[k : k + 1] for k in range(ITERS)]
    zero = jnp.zeros((1, 1), jnp.float32)
    padded = coef + [zero, zero]
    weights = []
    for i in range(VECS):
        value = 0.5 * padded[i + 1] - padded[i]
        if i == 0:
            value = value + 1.0
        elif i == 1:
            value = value + padded[0]
        else:
            value = value + 0.5 * padded[i - 1]
        weights.append(value)
    sums = [total[:, SUMS + k : SUMS + k + 1] for k in range(ITERS + 1)]
    mean = zero
    for k in range(ITERS):
        mean = mean + coef[k] * sums[k]
    mean = mean / count
    drift = sums[ITERS] / count
    column = jnp.concatenate(weights + [zero] * (16 - VECS), axis=0)
    row = jnp.zeros((1, LANES), jnp.float32)
    for i in range(VECS):
        row = jnp.where(lane[0:1] == i, weights[i], row)
    size = jnp.sum(jnp.sum(matrix * column * row, axis=1, keepdims=True), axis=0, keepdims=True)
    diagonal = jnp.sum(jnp.where(lane == sub, matrix, 0.0), axis=1, keepdims=True)
    spread = jnp.sum(jnp.abs(column) * jnp.sqrt(diagonal), axis=0, keepdims=True)
    flag[...] = jnp.broadcast_to(spread * spread / size, (8, LANES))

    def combine(z, carry):
        for block in range(rows // 8):
            out = 8 * block
            weight = metric[z, out : out + 8]
            inside = jnp.minimum(weight, 1.0)
            phi = inside * (-mean)
            rest = jnp.zeros((8, LANES), jnp.float32)
            for k in range(VECS):
                value = basis[k, z, out : out + 8]
                if k < ITERS:
                    phi = phi + coef[k] * value
                rest = rest + weights[k] * value
            solution_ref[z, out : out + 8] = phi
            residual_ref[z, out : out + 8] = weight * rest - inside * drift
        return carry

    lax.fori_loop(0, own_planes, combine, 0)


def f32(*shape):
    return jax.ShapeDtypeStruct(shape, jnp.float32)


def cyclic(count, shift):
    return [(i, (i + shift) % count) for i in range(count)]


def fast(potential, tissue_mask, layer_index, source):
    own_planes, rows, width = tissue_mask.shape
    gx, gy, gz = (lax.axis_size(name) for name in ("gx", "gy", "gz"))
    at_x, at_y, at_z = (lax.axis_index(name) for name in ("gx", "gy", "gz"))
    params = pltpu.CompilerParams(vmem_limit_bytes=60 * 1024 * 1024)
    stacked = jnp.stack([potential, source, tissue_mask.astype(jnp.float32)])

    full = gz * own_planes <= own_planes + 2 * HALO
    if full:
        planes = gz * own_planes
        first = at_z * own_planes
        fields, layers, offsets = [stacked], [layer_index], [first]
        for shift in range(1, gz):
            pairs = cyclic(gz, shift)
            fields.append(lax.ppermute(stacked, "gz", pairs))
            layers.append(lax.ppermute(layer_index, "gz", pairs))
            offsets.append(((at_z + gz - shift) % gz) * own_planes)
        own_number = 0
    else:
        planes = own_planes + 2 * HALO
        first = HALO
        fields, layers, offsets = [stacked], [layer_index], [HALO]
        own_number = 0
        left = HALO
        hop = 1
        while left > 0:
            size = min(left, own_planes)
            up = [(i, i + hop) for i in range(gz - hop)]
            down = [(j, i) for i, j in up]
            fields.append(lax.ppermute(stacked[:, own_planes - size :], "gz", up))
            layers.append(lax.ppermute(layer_index[own_planes - size :], "gz", up))
            offsets.append(left - size)
            fields.append(lax.ppermute(stacked[:, :size], "gz", down))
            layers.append(lax.ppermute(layer_index[:size], "gz", down))
            offsets.append(HALO + own_planes + HALO - left)
            left -= size
            hop += 1
    pieces = tuple(field.shape[1] for field in fields)
    offs = jnp.stack([jnp.asarray(o, jnp.int32) for o in offsets])
    groups = -(-planes // 8)
    y_rows = 3 * groups * rows + 8

    joined, to_left, to_right, sums = pl.pallas_call(
        functools.partial(pack_y, (pieces, own_number, planes, rows, full)),
        out_shape=(f32(3, planes, rows, LANES), f32(y_rows, LANES), f32(y_rows, LANES), f32(8, LANES)),
        in_specs=[SMEM] + [VMEM] * len(pieces),
        out_specs=(VMEM,) * 4,
        compiler_params=params,
        name="pack_y",
    )(offs, *fields)
    from_left = lax.ppermute(to_right, "gy", cyclic(gy, 1))
    from_right = lax.ppermute(to_left, "gy", cyclic(gy, gy - 1))
    others = [sums] + [lax.ppermute(sums, "gy", cyclic(gy, s)) for s in range(2, gy - 1)]

    x_size = x_rows(planes) + 8
    upper, lower, sums = pl.pallas_call(
        functools.partial(pack_x, (planes, rows, len(others))),
        out_shape=(f32(x_size, LANES), f32(x_size, LANES), f32(8, LANES)),
        in_specs=[VMEM] * (3 + len(others)),
        out_specs=(VMEM,) * 3,
        compiler_params=params,
        name="pack_x",
    )(joined, from_left, from_right, *others)
    from_upper = lax.ppermute(lower, "gx", cyclic(gx, 1))
    from_lower = lax.ppermute(upper, "gx", cyclic(gx, gx - 1))
    total = sums + from_upper[x_size - 8 :] + from_lower[x_size - 8 :]
    for s in range(2, gx - 1):
        total = total + lax.ppermute(sums, "gx", cyclic(gx, s))
    if not full:
        total = lax.psum(total, "gz")

    info = jnp.stack(
        [
            (at_y > 0).astype(jnp.int32),
            (at_y < gy - 1).astype(jnp.int32),
            (at_x > 0).astype(jnp.int32),
            (at_x < gx - 1).astype(jnp.int32),
            jnp.asarray(first, jnp.int32),
        ]
    )
    table = np.concatenate(
        [
            0.5 * tensor_table(LAYERS, bulk_long, bulk_trans),
            0.5 * tensor_table(LAYERS, intra_long, intra_trans),
        ],
        axis=1,
    ).reshape(-1)
    high = TOP + rows + 16
    grid = (2, planes + 2, high, LANES)
    rolled = sum(1 for offset in OFFSETS if offset[2])
    scratch = [
        pltpu.SMEM((planes + 2,), jnp.int32),
        pltpu.VMEM((3,) + grid, jnp.float32),
        pltpu.VMEM((3,) + grid, jnp.float32),
        pltpu.VMEM((len(OFFSETS),) + grid, jnp.float32),
        pltpu.VMEM((rolled,) + grid, jnp.float32),
        pltpu.VMEM((3,) + grid, jnp.float32),
        pltpu.VMEM((2,) + grid, jnp.float32),
        pltpu.VMEM((2,) + grid, jnp.float32),
        pltpu.VMEM(grid, jnp.float32),
        pltpu.VMEM(grid, jnp.float32),
        pltpu.VMEM((8, LANES), jnp.float32),
        pltpu.VMEM((-(-(SUMS + ITERS + 1) // 8) * 8, LANES), jnp.float32),
    ]
    sums_rows = scratch[-1].shape[0]
    gram, basis, metric, _ = pl.pallas_call(
        functools.partial(krylov, (pieces, planes, own_planes, rows, 0)),
        out_shape=(
            f32(8, sums_rows),
            f32(VECS, own_planes, rows, LANES),
            f32(own_planes, rows, LANES),
            f32(own_planes, rows, LANES),
        ),
        in_specs=[SMEM] * (3 + len(pieces)) + [VMEM] * 6,
        out_specs=(VMEM,) * 4,
        scratch_shapes=scratch,
        compiler_params=params,
        name="krylov",
    )(info, offs, jnp.asarray(table), *layers, joined, from_left, from_right, from_upper, from_lower, total)

    everyone = gx * gy * gz
    row = jnp.pad(gram[0:1], ((0, 0), (0, LANES - sums_rows)))
    gathered = lax.all_to_all(
        jnp.broadcast_to(row, (everyone, LANES)), ("gx", "gy", "gz"), 0, 0, tiled=True
    )
    answer, residual, flag = pl.pallas_call(
        functools.partial(finish, (own_planes, rows)),
        out_shape=(f32(own_planes, rows, LANES), f32(own_planes, rows, LANES), f32(8, LANES)),
        in_specs=[VMEM] * 4,
        out_specs=(VMEM,) * 3,
        compiler_params=params,
        name="finish",
    )(gathered, total, basis, metric)
    return answer, residual, flag


def body(potential, tissue_mask, layer_index, source):
    answer, residual, flag = fast(potential, tissue_mask, layer_index, source)
    return (answer, residual)


def solution(mesh):
    placed = (P("gz", "gx", "gy"), P("gz", "gx", "gy"), P("gz"), P("gz", "gx", "gy"))
    return jax.shard_map(
        body,
        mesh=mesh,
        in_specs=placed,
        out_specs=(P("gz", "gx", "gy"), P("gz", "gx", "gy")),
        check_vma=False,
    )
```

```python
import functools
import math

import jax
import jax.numpy as jnp
import numpy as np
from jax import lax
from jax.experimental import pallas as pl
from jax.experimental.pallas import tpu as pltpu
from jax.sharding import PartitionSpec as P

ITERS = 8
LAYERS = 16
HALO = ITERS + 1
LANES = 128
SLOT = 16
TOP = 16
LEAD = 2
CHUNK = 2
VECS = ITERS + 1
SUMS = VECS * VECS

OFFSETS = [
    (0, 1, 0),
    (0, 0, 1),
    (1, 0, 0),
    (0, 1, 1),
    (0, -1, 1),
    (1, 1, 0),
    (-1, 1, 0),
    (1, 0, 1),
    (-1, 0, 1),
]
bulk_long = 7.99
bulk_trans = 2.55
intra_long = 1.74
intra_trans = 0.19
bath_sigma = 5.0

VMEM = pl.BlockSpec(memory_space=pltpu.VMEM)
SMEM = pl.BlockSpec(memory_space=pltpu.SMEM)


def tensor_table(layers, longitudinal, transverse):
    depth = np.arange(layers, dtype=np.float64) / (layers - 1)
    helix = math.pi / 3.0 * (1.0 - 2.0 * depth)
    tilted = 0.35 * np.cos(math.pi * depth)
    fiber_x = np.cos(tilted) * np.cos(helix)
    fiber_y = np.cos(tilted) * np.sin(helix)
    fiber_z = np.sin(tilted)
    spread = longitudinal - transverse
    s_xx = transverse + spread * fiber_x * fiber_x
    s_yy = transverse + spread * fiber_y * fiber_y
    s_zz = transverse + spread * fiber_z * fiber_z
    s_xy = spread * fiber_x * fiber_y
    s_xz = spread * fiber_x * fiber_z
    s_yz = spread * fiber_y * fiber_z
    columns = [
        s_xx - np.abs(s_xy) - np.abs(s_xz),
        s_yy - np.abs(s_xy) - np.abs(s_yz),
        s_zz - np.abs(s_xz) - np.abs(s_yz),
        np.maximum(s_xy, 0.0),
        np.maximum(-s_xy, 0.0),
        np.maximum(s_xz, 0.0),
        np.maximum(-s_xz, 0.0),
        np.maximum(s_yz, 0.0),
        np.maximum(-s_yz, 0.0),
    ]
    return np.stack(columns, axis=1).astype(np.float32)


def lane_iota(shape):
    return lax.broadcasted_iota(jnp.int32, shape, len(shape) - 1)


def roll(value, shift, axis=-1):
    axis = axis % value.ndim
    shift = shift % value.shape[axis]
    return value if shift == 0 else pltpu.roll(value, shift, axis)


def pack_y(geometry, *refs):
    pieces, summed, rows = geometry
    piece_refs = refs[: len(pieces)]
    left, right, sums = refs[len(pieces) :]
    listed = [(ref, plane) for ref, length in zip(piece_refs, pieces) for plane in range(length)]
    groups = -(-len(listed) // 8)
    lane = lane_iota((rows, LANES))
    count = jnp.zeros((rows, LANES), jnp.float32)
    total = jnp.zeros((rows, LANES), jnp.float32)
    for ref, plane in listed[:summed]:
        inside = jnp.minimum(ref[2, plane], 1.0)
        count = count + inside
        total = total + inside * ref[1, plane]
    sums[...] = jnp.zeros((8, LANES), jnp.float32)
    sums[0:1] = jnp.sum(count, axis=0, keepdims=True)
    sums[1:2] = jnp.sum(total, axis=0, keepdims=True)
    for field in range(3):
        for group in range(groups):
            to_left = jnp.zeros((rows, LANES), jnp.float32)
            to_right = jnp.zeros((rows, LANES), jnp.float32)
            for slot, (ref, plane) in enumerate(listed[8 * group : 8 * group + 8]):
                value = ref[field, plane]
                here = (lane >= SLOT * slot) & (lane < SLOT * (slot + 1))
                to_left = jnp.where(here, roll(value, SLOT * slot), to_left)
                to_right = jnp.where(here, roll(value, SLOT * (slot + 1)), to_right)
            base = (field * groups + group) * rows
            left[base : base + rows] = to_left
            right[base : base + rows] = to_right
    last = 3 * groups * rows
    left[last : last + 8] = sums[...]
    right[last : last + 8] = sums[...]


class Strip:
    def __init__(self, planes):
        self.planes = planes
        self.groups = -(-planes // 8)
        self.side = 3 * planes * 8
        self.ninth = self.side + 2 * 3 * self.groups * 8
        self.side_ninth = self.ninth + 2 * 8 * self.groups
        self.sums = self.side_ninth + -(-4 * self.groups // 8) * 8
        self.rows = self.sums + 8

    def own(self, field, plane):
        return (field * self.planes + plane) * 8

    def edge(self, side, field, group):
        return self.side + ((side * 3 + field) * self.groups + group) * 8

    def own_ninth(self, kind, group):
        return self.ninth + (kind * self.groups + group) * 8

    def edge_ninth(self, side, kind, group):
        return self.side_ninth + (side * 2 + kind) * self.groups + group


def pack_x(geometry, *refs):
    pieces, rows, others = geometry
    piece_refs = refs[: len(pieces)]
    from_left, from_right = refs[len(pieces) : len(pieces) + 2]
    other_refs = refs[len(pieces) + 2 : len(pieces) + 2 + others]
    upper, lower, sums = refs[len(pieces) + 2 + others :]
    listed = [(ref, plane) for ref, length in zip(piece_refs, pieces) for plane in range(length)]
    strip = Strip(len(listed))
    last = 3 * strip.groups * rows
    total = from_left[last : last + 8] + from_right[last : last + 8]
    for ref in other_refs:
        total = total + ref[...]
    sums[...] = total
    for out, first, ninth in ((upper, 0, 8), (lower, rows - 8, rows - 9)):
        out[strip.ninth : strip.sums] = jnp.zeros((strip.sums - strip.ninth, LANES), jnp.float32)
        out[strip.sums : strip.rows] = total
        for number, (ref, plane) in enumerate(listed):
            for field in range(3):
                at = strip.own(field, number)
                out[at : at + 8] = ref[field, plane, first : first + 8]
            for kind, field in enumerate((0, 2)):
                at = strip.own_ninth(kind, number // 8) + number % 8
                out[at : at + 1] = ref[field, plane, ninth : ninth + 1]
        for side, packed in enumerate((from_left, from_right)):
            for group in range(strip.groups):
                for field in range(3):
                    at = strip.edge(side, field, group)
                    base = (field * strip.groups + group) * rows
                    out[at : at + 8] = packed[base + first : base + first + 8]
                for kind, field in enumerate((0, 2)):
                    at = strip.edge_ninth(side, kind, group)
                    base = (field * strip.groups + group) * rows
                    out[at : at + 1] = packed[base + ninth : base + ninth + 1]


def krylov(geometry, table, *refs):
    pieces, planes, own_planes, rows, extras, full, gz, gy = geometry
    layer_refs = refs[: len(pieces)]
    refs = refs[len(pieces) :]
    piece_refs = refs[: len(pieces)]
    refs = refs[len(pieces) :]
    from_left, from_right, from_upper, from_lower, own_sums = refs[:5]
    extra_refs = refs[5 : 5 + extras]
    refs = refs[5 + extras :]
    gram, basis, metric, total_out = refs[:4]
    layer, pot, med, src, edge, vec, vec_l, jac, kap, met, rowsum = refs[4:]
    high = TOP + rows + 16
    inner = (rows + 16) // 8
    both = (0, 1)
    strip = Strip(planes)
    groups = strip.groups
    lane = lane_iota((8, LANES))
    zero = jnp.zeros((8, LANES), jnp.float32)
    at_z = lax.axis_index("gz")
    at_y = lax.axis_index("gy")
    keep_left = jnp.where(at_y > 0, 1.0, 0.0)
    keep_right = jnp.where(at_y < gy - 1, 1.0, 0.0)

    if full:
        offsets = [lax.rem(at_z + gz - shift, gz) * own_planes for shift in range(gz)]
        first = offsets[0]
    else:
        offsets = [HALO]
        left = HALO
        for size in pieces[1::2]:
            offsets += [left - size, HALO + own_planes + HALO - left]
            left -= size
        first = HALO
    listed = [
        (ref, plane, offset + plane)
        for ref, length, offset in zip(piece_refs, pieces, offsets)
        for plane in range(length)
    ]
    layer[0] = 0
    layer[planes + 1] = 0
    for number, length in enumerate(pieces):
        for plane in range(length):
            layer[offsets[number] + plane + 1] = layer_refs[number][plane]

    totals = own_sums[...]
    if extras:
        totals = totals + from_upper[strip.sums : strip.rows] + from_lower[strip.sums : strip.rows]
    for ref in extra_refs:
        totals = totals + ref[...]
    total_out[...] = totals
    mean = jnp.sum(totals[1:2], axis=1, keepdims=True) / jnp.sum(
        totals[0:1], axis=1, keepdims=True
    )

    outside = (LEAD - 1, LEAD + planes)
    for plane in outside:
        for tile in both:
            for at in range(0, high, 8):
                for copy in both:
                    pot[copy, tile, plane, at : at + 8] = zero
                    med[copy, tile, plane, at : at + 8] = zero
                    vec_l[copy, tile, plane, at : at + 8] = zero
                for slot in range(VECS + 1):
                    vec[slot, tile, plane, at : at + 8] = zero
                for column, (dz, _, _) in enumerate(OFFSETS):
                    if dz:
                        edge[column, tile, plane, at : at + 8] = zero

    def tiles_of(own, strip_l, strip_r, slot, kind):
        ln = lane_iota(own.shape)
        a = roll(strip_l, LANES - SLOT * slot)
        b = roll(strip_r, LANES - SLOT * (slot + 1))
        if kind == 2:
            a, b = a * keep_left, b * keep_right
        low = jnp.where(ln < SLOT, a, roll(own, SLOT))
        up = jnp.where(ln >= LANES - SLOT, b, roll(own, LANES - SLOT))
        return low, up

    targets = {0: pot, 1: src, 2: med}

    def place(kind, tile, plane, at, value):
        size = value.shape[0]
        if kind == 1:
            src[tile, plane, at : at + size] = value
        else:
            targets[kind][0, tile, plane, at : at + size] = value
            targets[kind][1, tile, plane, at : at + size] = roll(value, LANES - 1)

    for number, (ref, plane, z) in enumerate(listed):
        group, slot = divmod(number, 8)
        for field in range(3):
            base = (field * groups + group) * rows
            own = (
                ref[field, plane],
                from_left[base : base + rows],
                from_right[base : base + rows],
            )
            for tile, value in enumerate(tiles_of(*own, slot, field)):
                place(field, tile, z + LEAD, TOP, value)
            for packed, at in ((from_upper, TOP - 8), (from_lower, TOP + rows)):
                r0 = strip.own(field, number)
                r1 = strip.edge(0, field, group)
                r2 = strip.edge(1, field, group)
                halo = (packed[r0 : r0 + 8], packed[r1 : r1 + 8], packed[r2 : r2 + 8])
                for tile, value in enumerate(tiles_of(*halo, slot, field)):
                    place(field, tile, z + LEAD, at, value)
        for kind, field in enumerate((0, 2)):
            for packed, block, at in (
                (from_upper, 0, TOP - HALO),
                (from_lower, high - 8, TOP + rows + 8),
            ):
                r0 = strip.own_ninth(kind, group) + slot
                r1 = strip.edge_ninth(0, kind, group)
                r2 = strip.edge_ninth(1, kind, group)
                halo = (packed[r0 : r0 + 1], packed[r1 : r1 + 1], packed[r2 : r2 + 1])
                for tile, value in enumerate(tiles_of(*halo, slot, field)):
                    for copy in both:
                        targets[field][copy, tile, z + LEAD, block : block + 8] = zero
                    place(field, tile, z + LEAD, at, value)

    def edges_of(z, carry):
        here = layer[z + 1] * 18
        there = {d: layer[z + 1 + d] * 18 for d in (-1, 0, 1)}
        own_g = [table[here + c] for c in range(9)]
        next_g = [table[there[o[0]] + c] for c, o in enumerate(OFFSETS)]
        flow_g = [table[here + 9 + c] + table[there[o[0]] + 9 + c] for c, o in enumerate(OFFSETS)]
        for tile in both:
            for block in range(inner + 2):
                at = 8 * block
                m = med[0, tile, z + LEAD, at : at + 8]
                v = pot[0, tile, z + LEAD, at : at + 8]
                inside = jnp.minimum(m, 1.0)
                tissue = jnp.maximum(m - 1.0, 0.0)
                bath = (inside - tissue) * (0.5 * bath_sigma)
                for column, (dz, dx, dy) in enumerate(OFFSETS):
                    if block == (0 if dx < 0 else inner + 1):
                        continue
                    row = at + dx
                    n = med[dy, tile, z + LEAD + dz, row : row + 8]
                    w = pot[dy, tile, z + LEAD + dz, row : row + 8]
                    n_in = jnp.minimum(n, 1.0)
                    n_ti = jnp.maximum(n - 1.0, 0.0)
                    mine = tissue * own_g[column]
                    other = n_ti * next_g[column]
                    if column < 3:
                        mine = mine + bath
                        other = other + (n_in - n_ti) * (0.5 * bath_sigma)
                    edge[column, tile, z + LEAD, at : at + 8] = n_in * mine + inside * other
                    vec[column, tile, z + LEAD, at : at + 8] = (
                        (tissue * n_ti) * flow_g[column]
                    ) * (w - v)
        return carry

    lax.fori_loop(0, planes, edges_of, 0)

    def lift(slot, side, z):
        for plane in range(CHUNK):
            for tile in both:
                for block in range(inner):
                    at = 8 + 8 * block
                    vec_l[side, tile, z + plane + LEAD, at : at + 8] = roll(
                        vec[slot, tile, z + plane + LEAD, at : at + 8], LANES - 1
                    )

    slot_of = lambda number: number - 1 if number else VECS

    def start_of(step, carry):
        base = step * CHUNK
        lift(slot_of(0), 0, base - CHUNK)
        for tile in both:
            for plane in range(CHUNK):
                z = base + plane
                for block in range(inner):
                    at = 8 + 8 * block
                    late_e, late_f = zero, zero
                    diagonal, flow = zero, zero
                    for column, (dz, dx, dy) in enumerate(OFFSETS):
                        back = (tile, z + LEAD - dz, slice(at - dx, at - dx + 8))
                        e = edge[(column,) + back]
                        f = vec[(column,) + back]
                        if dy:
                            late_e, late_f = late_e + e, late_f + f
                        else:
                            diagonal, flow = diagonal + e, flow - f
                        diagonal = diagonal + edge[column, tile, z + LEAD, at : at + 8]
                        flow = flow + vec[column, tile, z + LEAD, at : at + 8]
                    diagonal = diagonal + roll(late_e, 1)
                    flow = flow - roll(late_f, 1)
                    inside = jnp.minimum(med[0, tile, z + LEAD, at : at + 8], 1.0)
                    residual = flow + inside * (src[tile, z + LEAD, at : at + 8] - mean)
                    size = jnp.maximum(diagonal, 1.0)
                    scale = inside / size
                    jac[tile, z + LEAD, at : at + 8] = scale
                    kap[tile, z + LEAD, at : at + 8] = jnp.maximum(inside - diagonal, 0.0)
                    met[tile, z + LEAD, at : at + 8] = inside * size
                    vec[slot_of(0), tile, z + LEAD, at : at + 8] = scale * residual
        return carry

    lax.fori_loop(0, planes // CHUNK, start_of, 0)
    lift(slot_of(0), 0, planes - CHUNK)

    for step in range(ITERS):
        now, later, before = slot_of(step), slot_of(step + 1), slot_of(max(step - 1, 0))
        side, side_next = step % 2, (step + 1) % 2
        reach = ITERS - 1 - step
        low = jnp.maximum(first - reach, 0) // CHUNK
        up = (jnp.minimum(first + own_planes + reach, planes) + CHUNK - 1) // CHUNK

        def apply(number, carry):
            base = number * CHUNK
            if step + 1 < ITERS:
                lift(later, side_next, base - CHUNK)
            for tile in both:
                for block in range(inner):
                    at = 8 + 8 * block
                    for plane in range(CHUNK):
                        z = base + plane
                        total, late = zero, zero
                        for column, (dz, dx, dy) in enumerate(OFFSETS):
                            back = (tile, z + LEAD - dz, slice(at - dx, at - dx + 8))
                            product = edge[(column,) + back] * vec[(now,) + back]
                            if dy:
                                late = late + product
                            else:
                                total = total + product
                            ahead = (tile, z + LEAD + dz, slice(at + dx, at + dx + 8))
                            value = vec_l[(side,) + ahead] if dy else vec[(now,) + ahead]
                            total = total + edge[column, tile, z + LEAD, at : at + 8] * value
                        cell = (tile, z + LEAD, slice(at, at + 8))
                        total = total + kap[cell] * vec[(now,) + cell]
                        value = jac[cell] * (total + roll(late, 1))
                        if step:
                            value = 2.0 * value - vec[(before,) + cell]
                        vec[(later,) + cell] = value
            return carry

        lax.fori_loop(low, up, apply, 0)
        if step + 1 < ITERS:
            lift(later, side_next, (up - 1) * CHUNK)

    def joined(value):
        low = roll(value[0], LANES - SLOT)
        up = roll(value[1], SLOT)
        return jnp.where(lane < LANES // 2, low, up)

    def own_of(number, carry):
        for plane in range(CHUNK):
            z = number * CHUNK + plane
            for block in range(rows // 8):
                at = TOP + 8 * block
                out = 8 * block
                cell = lambda tile: (tile, first + z + LEAD, slice(at, at + 8))
                metric[z, out : out + 8] = joined([met[cell(tile)] for tile in both])
                for index in range(VECS):
                    basis[index, z, out : out + 8] = joined(
                        [vec[(slot_of(index),) + cell(tile)] for tile in both]
                    )
        return carry

    lax.fori_loop(0, own_planes // CHUNK, own_of, 0)

    pairs = [(i, j) for i in range(VECS) for j in range(i, VECS)]
    half = 26
    rowsum[...] = jnp.zeros(rowsum.shape, jnp.float32)
    for part, plain in ((pairs[:half], False), (pairs[half:], True)):

        def gather(z, carry):
            carry = list(carry)
            for block in range(rows // 8):
                out = 8 * block
                weight = metric[z, out : out + 8]
                used = range(VECS) if plain else sorted({k for pair in part for k in pair})
                loaded = {k: basis[k, z, out : out + 8] for k in used}
                scaled = {i: loaded[i] * weight for i in {i for i, _ in part} | ({0} if plain else set())}
                for number, (i, j) in enumerate(part):
                    carry[number] = carry[number] + scaled[i] * loaded[j]
                if plain:
                    for k in range(ITERS):
                        carry[len(part) + k] = carry[len(part) + k] + loaded[k]
                    carry[-1] = carry[-1] + scaled[0]
            return tuple(carry)

        count = len(part) + (ITERS + 1 if plain else 0)
        done = lax.fori_loop(0, own_planes, gather, tuple(zero for _ in range(count)))
        done = [jnp.sum(value, axis=0, keepdims=True) for value in done]
        for (i, j), value in zip(part, done):
            rowsum[VECS * i + j : VECS * i + j + 1] = value
            if i != j:
                rowsum[VECS * j + i : VECS * j + i + 1] = value
        for k, value in enumerate(done[len(part) :]):
            rowsum[SUMS + k : SUMS + k + 1] = value
    row = lax.dot_general(
        jnp.ones((8, LANES), jnp.float32),
        rowsum[...],
        (((1,), (1,)), ((), ())),
        precision=lax.Precision.HIGHEST,
        preferred_element_type=jnp.float32,
    )
    for at in range(0, gram.shape[0], 8):
        gram[at : at + 8] = row


def finish(geometry, gathered, total_in, basis, metric, solution_ref, residual_ref, flag):
    own_planes, rows = geometry
    total = jnp.sum(gathered[...], axis=0, keepdims=True)
    count = jnp.sum(total_in[0:1], axis=1, keepdims=True)
    lane = lane_iota((16, LANES))
    sub = lax.broadcasted_iota(jnp.int32, (16, LANES), 0)
    matrix = jnp.zeros((16, LANES), jnp.float32)
    for i in range(VECS):
        line = roll(total, LANES - VECS * i)
        matrix = jnp.where(sub == i, jnp.broadcast_to(line, (16, LANES)), matrix)
    matrix = jnp.where(lane < VECS, matrix, 0.0)
    reflected = jnp.where(lane == 0, roll(matrix, LANES - 1), roll(matrix, 1))
    square = matrix - 0.5 * (roll(matrix, LANES - 1) + reflected)
    system = jnp.where(lane < ITERS, square, 0.0)
    system = jnp.where(lane == ITERS, roll(matrix, ITERS), system)[0:8]
    lane8 = lane[0:8]
    sub8 = sub[0:8]
    for k in range(ITERS):
        line = system[k : k + 1]
        pivot = jnp.sum(jnp.where(lane8[0:1] == k, line, 0.0), axis=1, keepdims=True)
        line = line / pivot
        column = jnp.sum(jnp.where(lane8 == k, system, 0.0), axis=1, keepdims=True)
        line8 = jnp.broadcast_to(line, (8, LANES))
        system = jnp.where(sub8 == k, line8, system - column * line8)
    answer = jnp.sum(jnp.where(lane8 == ITERS, system, 0.0), axis=1, keepdims=True)
    coef = [answer[k : k + 1] for k in range(ITERS)]
    zero = jnp.zeros((1, 1), jnp.float32)
    padded = coef + [zero, zero]
    weights = []
    for i in range(VECS):
        value = 0.5 * padded[i + 1] - padded[i]
        if i == 0:
            value = value + 1.0
        elif i == 1:
            value = value + padded[0]
        else:
            value = value + 0.5 * padded[i - 1]
        weights.append(value)
    sums = [total[:, SUMS + k : SUMS + k + 1] for k in range(ITERS + 1)]
    mean = zero
    for k in range(ITERS):
        mean = mean + coef[k] * sums[k]
    mean = mean / count
    drift = sums[ITERS] / count
    column = jnp.concatenate(weights + [zero] * (16 - VECS), axis=0)
    row = jnp.zeros((1, LANES), jnp.float32)
    for i in range(VECS):
        row = jnp.where(lane[0:1] == i, weights[i], row)
    size = jnp.sum(jnp.sum(matrix * column * row, axis=1, keepdims=True), axis=0, keepdims=True)
    diagonal = jnp.sum(jnp.where(lane == sub, matrix, 0.0), axis=1, keepdims=True)
    spread = jnp.sum(jnp.abs(column) * jnp.sqrt(diagonal), axis=0, keepdims=True)
    flag[...] = jnp.broadcast_to(spread * spread / size, (8, LANES))

    def combine(z, carry):
        for block in range(rows // 8):
            out = 8 * block
            weight = metric[z, out : out + 8]
            inside = jnp.minimum(weight, 1.0)
            phi = inside * (-mean)
            rest = jnp.zeros((8, LANES), jnp.float32)
            for k in range(VECS):
                value = basis[k, z, out : out + 8]
                if k < ITERS:
                    phi = phi + coef[k] * value
                rest = rest + weights[k] * value
            solution_ref[z, out : out + 8] = phi
            residual_ref[z, out : out + 8] = weight * rest - inside * drift
        return carry

    lax.fori_loop(0, own_planes, combine, 0)


def f32(*shape):
    return jax.ShapeDtypeStruct(shape, jnp.float32)


def cyclic(count, shift):
    return [(i, (i + shift) % count) for i in range(count)]


def fast(potential, tissue_mask, layer_index, source):
    own_planes, rows, width = tissue_mask.shape
    gx, gy, gz = (lax.axis_size(name) for name in ("gx", "gy", "gz"))
    params = pltpu.CompilerParams(vmem_limit_bytes=60 * 1024 * 1024)
    stacked = jnp.stack([potential, source, tissue_mask.astype(jnp.float32)])

    full = gz * own_planes <= own_planes + 2 * HALO
    fields, layers = [stacked], [layer_index]
    if full:
        planes = gz * own_planes
        for shift in range(1, gz):
            fields.append(lax.ppermute(stacked, "gz", cyclic(gz, shift)))
            layers.append(lax.ppermute(layer_index, "gz", cyclic(gz, shift)))
    else:
        planes = own_planes + 2 * HALO
        left, hop = HALO, 1
        while left > 0:
            size = min(left, own_planes)
            up = [(i, i + hop) for i in range(gz - hop)]
            down = [(j, i) for i, j in up]
            fields.append(lax.ppermute(stacked[:, own_planes - size :], "gz", up))
            layers.append(lax.ppermute(layer_index[own_planes - size :], "gz", up))
            fields.append(lax.ppermute(stacked[:, :size], "gz", down))
            layers.append(lax.ppermute(layer_index[:size], "gz", down))
            left -= size
            hop += 1
    pieces = tuple(field.shape[1] for field in fields)
    summed = planes if full else own_planes
    groups = -(-planes // 8)
    y_rows = 3 * groups * rows + 8

    to_left, to_right, sums = pl.pallas_call(
        functools.partial(pack_y, (pieces, summed, rows)),
        out_shape=(f32(y_rows, LANES), f32(y_rows, LANES), f32(8, LANES)),
        in_specs=[VMEM] * len(pieces),
        out_specs=(VMEM,) * 3,
        compiler_params=params,
        name="pack_y",
    )(*fields)
    from_left = lax.ppermute(to_right, "gy", cyclic(gy, 1))
    from_right = lax.ppermute(to_left, "gy", cyclic(gy, gy - 1))
    others = [sums] + [lax.ppermute(sums, "gy", cyclic(gy, s)) for s in range(2, gy - 1)]

    strip = Strip(planes)
    upper, lower, sums = pl.pallas_call(
        functools.partial(pack_x, (pieces, rows, len(others))),
        out_shape=(f32(strip.rows, LANES), f32(strip.rows, LANES), f32(8, LANES)),
        in_specs=[VMEM] * (len(pieces) + 2 + len(others)),
        out_specs=(VMEM,) * 3,
        compiler_params=params,
        name="pack_x",
    )(*fields, from_left, from_right, *others)
    forth = [(i, i + 1) for i in range(gx - 1)]
    from_upper = lax.ppermute(lower, "gx", forth)
    from_lower = lax.ppermute(upper, "gx", [(j, i) for i, j in forth])
    extra = [lax.ppermute(sums, "gx", cyclic(gx, s)) for s in range(2, gx - 1)]
    extra.append(lax.ppermute(sums, "gx", [(0, gx - 1), (gx - 1, 0)]))
    if not full:
        sums = sums + from_upper[strip.sums :] + from_lower[strip.sums :] + sum(extra)
        sums = lax.psum(sums, "gz")
        extra = []

    table = np.concatenate(
        [
            0.5 * tensor_table(LAYERS, bulk_long, bulk_trans),
            0.5 * tensor_table(LAYERS, intra_long, intra_trans),
        ],
        axis=1,
    ).reshape(-1)
    high = TOP + rows + 16
    grid = (2, planes + LEAD + 1, high, LANES)
    everyone = gx * gy * gz
    gram, basis, metric, total = pl.pallas_call(
        functools.partial(krylov, (pieces, planes, own_planes, rows, len(extra), full, gz, gy)),
        out_shape=(
            f32(everyone, LANES),
            f32(VECS, own_planes, rows, LANES),
            f32(own_planes, rows, LANES),
            f32(8, LANES),
        ),
        in_specs=[SMEM] * (1 + len(pieces)) + [VMEM] * (len(pieces) + 5 + len(extra)),
        out_specs=(VMEM,) * 4,
        scratch_shapes=[
            pltpu.SMEM((planes + 2,), jnp.int32),
            pltpu.VMEM((2,) + grid, jnp.float32),
            pltpu.VMEM((2,) + grid, jnp.float32),
            pltpu.VMEM(grid, jnp.float32),
            pltpu.VMEM((len(OFFSETS),) + grid, jnp.float32),
            pltpu.VMEM((VECS + 1,) + grid, jnp.float32),
            pltpu.VMEM((2,) + grid, jnp.float32),
            pltpu.VMEM(grid, jnp.float32),
            pltpu.VMEM(grid, jnp.float32),
            pltpu.VMEM(grid, jnp.float32),
            pltpu.VMEM((LANES, LANES), jnp.float32),
        ],
        compiler_params=params,
        name="krylov",
    )(
        jnp.asarray(table),
        *layers,
        *fields,
        from_left,
        from_right,
        from_upper,
        from_lower,
        sums,
        *extra,
    )
    gathered = lax.all_to_all(gram, ("gx", "gy", "gz"), 0, 0, tiled=True)
    answer, residual, flag = pl.pallas_call(
        functools.partial(finish, (own_planes, rows)),
        out_shape=(f32(own_planes, rows, LANES), f32(own_planes, rows, LANES), f32(8, LANES)),
        in_specs=[VMEM] * 4,
        out_specs=(VMEM,) * 3,
        compiler_params=params,
        name="finish",
    )(gathered, total, basis, metric)
    return answer, residual, flag


def body(potential, tissue_mask, layer_index, source):
    answer, residual, flag = fast(potential, tissue_mask, layer_index, source)
    return (answer, residual)


def solution(mesh):
    placed = (P("gz", "gx", "gy"), P("gz", "gx", "gy"), P("gz"), P("gz", "gx", "gy"))
    return jax.shard_map(
        body,
        mesh=mesh,
        in_specs=placed,
        out_specs=(P("gz", "gx", "gy"), P("gz", "gx", "gy")),
        check_vma=False,
    )
```

```python
import functools
import math

import jax
import jax.numpy as jnp
import numpy as np
from jax import lax
from jax.experimental import pallas as pl
from jax.experimental.pallas import tpu as pltpu
from jax.sharding import PartitionSpec as P

ITERS = 8
LAYERS = 16
HALO = ITERS + 1
LANES = 128
SLOT = 16
TOP = 16
LEAD = 2
CHUNK = 2
VECS = ITERS + 1
SUMS = VECS * VECS

OFFSETS = [
    (0, 1, 0),
    (0, 0, 1),
    (1, 0, 0),
    (0, 1, 1),
    (0, -1, 1),
    (1, 1, 0),
    (-1, 1, 0),
    (1, 0, 1),
    (-1, 0, 1),
]
bulk_long = 7.99
bulk_trans = 2.55
intra_long = 1.74
intra_trans = 0.19
bath_sigma = 5.0

VMEM = pl.BlockSpec(memory_space=pltpu.VMEM)
SMEM = pl.BlockSpec(memory_space=pltpu.SMEM)


def tensor_table(layers, longitudinal, transverse):
    depth = np.arange(layers, dtype=np.float64) / (layers - 1)
    helix = math.pi / 3.0 * (1.0 - 2.0 * depth)
    tilted = 0.35 * np.cos(math.pi * depth)
    fiber_x = np.cos(tilted) * np.cos(helix)
    fiber_y = np.cos(tilted) * np.sin(helix)
    fiber_z = np.sin(tilted)
    spread = longitudinal - transverse
    s_xx = transverse + spread * fiber_x * fiber_x
    s_yy = transverse + spread * fiber_y * fiber_y
    s_zz = transverse + spread * fiber_z * fiber_z
    s_xy = spread * fiber_x * fiber_y
    s_xz = spread * fiber_x * fiber_z
    s_yz = spread * fiber_y * fiber_z
    columns = [
        s_xx - np.abs(s_xy) - np.abs(s_xz),
        s_yy - np.abs(s_xy) - np.abs(s_yz),
        s_zz - np.abs(s_xz) - np.abs(s_yz),
        np.maximum(s_xy, 0.0),
        np.maximum(-s_xy, 0.0),
        np.maximum(s_xz, 0.0),
        np.maximum(-s_xz, 0.0),
        np.maximum(s_yz, 0.0),
        np.maximum(-s_yz, 0.0),
    ]
    return np.stack(columns, axis=1).astype(np.float32)


def lane_iota(shape):
    return lax.broadcasted_iota(jnp.int32, shape, len(shape) - 1)


def roll(value, shift, axis=-1):
    axis = axis % value.ndim
    shift = shift % value.shape[axis]
    return value if shift == 0 else pltpu.roll(value, shift, axis)


def pack_y(geometry, *refs):
    pieces, summed, rows = geometry
    piece_refs = refs[: len(pieces)]
    left, right, sums = refs[len(pieces) :]
    listed = [(ref, plane) for ref, length in zip(piece_refs, pieces) for plane in range(length)]
    groups = -(-len(listed) // 8)
    lane = lane_iota((rows, LANES))
    count = jnp.zeros((rows, LANES), jnp.float32)
    total = jnp.zeros((rows, LANES), jnp.float32)
    for ref, plane in listed[:summed]:
        inside = jnp.minimum(ref[2, plane], 1.0)
        count = count + inside
        total = total + inside * ref[1, plane]
    sums[...] = jnp.zeros((8, LANES), jnp.float32)
    sums[0:1] = jnp.sum(count, axis=0, keepdims=True)
    sums[1:2] = jnp.sum(total, axis=0, keepdims=True)
    for field in range(3):
        for group in range(groups):
            to_left = jnp.zeros((rows, LANES), jnp.float32)
            to_right = jnp.zeros((rows, LANES), jnp.float32)
            for slot, (ref, plane) in enumerate(listed[8 * group : 8 * group + 8]):
                value = ref[field, plane]
                here = (lane >= SLOT * slot) & (lane < SLOT * (slot + 1))
                to_left = jnp.where(here, roll(value, SLOT * slot), to_left)
                to_right = jnp.where(here, roll(value, SLOT * (slot + 1)), to_right)
            base = (field * groups + group) * rows
            left[base : base + rows] = to_left
            right[base : base + rows] = to_right
    last = 3 * groups * rows
    left[last : last + 8] = sums[...]
    right[last : last + 8] = sums[...]


class Strip:
    def __init__(self, planes):
        self.planes = planes
        self.groups = -(-planes // 8)
        self.side = 3 * planes * 8
        self.ninth = self.side + 2 * 3 * self.groups * 8
        self.side_ninth = self.ninth + 2 * 8 * self.groups
        self.sums = self.side_ninth + -(-4 * self.groups // 8) * 8
        self.rows = self.sums + 8

    def own(self, field, plane):
        return (field * self.planes + plane) * 8

    def edge(self, side, field, group):
        return self.side + ((side * 3 + field) * self.groups + group) * 8

    def own_ninth(self, kind, group):
        return self.ninth + (kind * self.groups + group) * 8

    def edge_ninth(self, side, kind, group):
        return self.side_ninth + (side * 2 + kind) * self.groups + group


def pack_x(geometry, *refs):
    pieces, rows = geometry
    piece_refs = refs[: len(pieces)]
    from_left, from_right, total_ref, upper, lower = refs[len(pieces) :]
    listed = [(ref, plane) for ref, length in zip(piece_refs, pieces) for plane in range(length)]
    strip = Strip(len(listed))
    total = total_ref[...]
    for out, first, ninth in ((upper, 0, 8), (lower, rows - 8, rows - 9)):
        out[strip.ninth : strip.sums] = jnp.zeros((strip.sums - strip.ninth, LANES), jnp.float32)
        out[strip.sums : strip.rows] = total
        for number, (ref, plane) in enumerate(listed):
            for field in range(3):
                at = strip.own(field, number)
                out[at : at + 8] = ref[field, plane, first : first + 8]
            for kind, field in enumerate((0, 2)):
                at = strip.own_ninth(kind, number // 8) + number % 8
                out[at : at + 1] = ref[field, plane, ninth : ninth + 1]
        for side, packed in enumerate((from_left, from_right)):
            for group in range(strip.groups):
                for field in range(3):
                    at = strip.edge(side, field, group)
                    base = (field * strip.groups + group) * rows
                    out[at : at + 8] = packed[base + first : base + first + 8]
                for kind, field in enumerate((0, 2)):
                    at = strip.edge_ninth(side, kind, group)
                    base = (field * strip.groups + group) * rows
                    out[at : at + 1] = packed[base + ninth : base + ninth + 1]


def krylov(geometry, table, *refs):
    pieces, planes, own_planes, rows, extras, full, gz, gy = geometry
    layer_refs = refs[: len(pieces)]
    refs = refs[len(pieces) :]
    piece_refs = refs[: len(pieces)]
    refs = refs[len(pieces) :]
    from_left, from_right, from_upper, from_lower, own_sums = refs[:5]
    extra_refs = refs[5 : 5 + extras]
    refs = refs[5 + extras :]
    gram, basis, metric, total_out = refs[:4]
    layer, pot, med, src, edge, vec, vec_l, jac, kap, met, rowsum = refs[4:]
    high = TOP + rows + 16
    inner = (rows + 16) // 8
    both = (0, 1)
    strip = Strip(planes)
    groups = strip.groups
    lane = lane_iota((8, LANES))
    zero = jnp.zeros((8, LANES), jnp.float32)
    at_z = lax.axis_index("gz")
    at_y = lax.axis_index("gy")
    keep_left = jnp.where(at_y > 0, 1.0, 0.0)
    keep_right = jnp.where(at_y < gy - 1, 1.0, 0.0)

    if full:
        offsets = [lax.rem(at_z + gz - shift, gz) * own_planes for shift in range(gz)]
        first = offsets[0]
    else:
        offsets = [HALO]
        left = HALO
        for size in pieces[1::2]:
            offsets += [left - size, HALO + own_planes + HALO - left]
            left -= size
        first = HALO
    listed = [
        (ref, plane, offset + plane)
        for ref, length, offset in zip(piece_refs, pieces, offsets)
        for plane in range(length)
    ]
    layer[0] = 0
    layer[planes + 1] = 0
    for number, length in enumerate(pieces):
        for plane in range(length):
            layer[offsets[number] + plane + 1] = layer_refs[number][plane]

    totals = own_sums[...]
    if extras:
        totals = totals + from_upper[strip.sums : strip.rows] + from_lower[strip.sums : strip.rows]
    for ref in extra_refs:
        totals = totals + ref[...]
    total_out[...] = totals
    mean = jnp.sum(totals[1:2], axis=1, keepdims=True) / jnp.sum(
        totals[0:1], axis=1, keepdims=True
    )

    outside = (LEAD - 1, LEAD + planes)
    for plane in outside:
        for tile in both:
            for at in range(0, high, 8):
                for copy in both:
                    pot[copy, tile, plane, at : at + 8] = zero
                    med[copy, tile, plane, at : at + 8] = zero
                    vec_l[copy, tile, plane, at : at + 8] = zero
                for slot in range(VECS + 1):
                    vec[slot, tile, plane, at : at + 8] = zero
                for column, (dz, _, _) in enumerate(OFFSETS):
                    if dz:
                        edge[column, tile, plane, at : at + 8] = zero

    def tiles_of(own, strip_l, strip_r, slot, kind):
        ln = lane_iota(own.shape)
        a = roll(strip_l, LANES - SLOT * slot)
        b = roll(strip_r, LANES - SLOT * (slot + 1))
        if kind == 2:
            a, b = a * keep_left, b * keep_right
        low = jnp.where(ln < SLOT, a, roll(own, SLOT))
        up = jnp.where(ln >= LANES - SLOT, b, roll(own, LANES - SLOT))
        return low, up

    targets = {0: pot, 1: src, 2: med}

    def place(kind, tile, plane, at, value):
        size = value.shape[0]
        if kind == 1:
            src[tile, plane, at : at + size] = value
        else:
            targets[kind][0, tile, plane, at : at + size] = value

    for number, (ref, plane, z) in enumerate(listed):
        group, slot = divmod(number, 8)
        for field in range(3):
            base = (field * groups + group) * rows
            own = (
                ref[field, plane],
                from_left[base : base + rows],
                from_right[base : base + rows],
            )
            for tile, value in enumerate(tiles_of(*own, slot, field)):
                place(field, tile, z + LEAD, TOP, value)
            for packed, at in ((from_upper, TOP - 8), (from_lower, TOP + rows)):
                r0 = strip.own(field, number)
                r1 = strip.edge(0, field, group)
                r2 = strip.edge(1, field, group)
                halo = (packed[r0 : r0 + 8], packed[r1 : r1 + 8], packed[r2 : r2 + 8])
                for tile, value in enumerate(tiles_of(*halo, slot, field)):
                    place(field, tile, z + LEAD, at, value)
        for kind, field in enumerate((0, 2)):
            for packed, block, at in (
                (from_upper, 0, TOP - HALO),
                (from_lower, high - 8, TOP + rows + 8),
            ):
                r0 = strip.own_ninth(kind, group) + slot
                r1 = strip.edge_ninth(0, kind, group)
                r2 = strip.edge_ninth(1, kind, group)
                halo = (packed[r0 : r0 + 1], packed[r1 : r1 + 1], packed[r2 : r2 + 1])
                for tile, value in enumerate(tiles_of(*halo, slot, field)):
                    targets[field][0, tile, z + LEAD, block : block + 8] = zero
                    place(field, tile, z + LEAD, at, value)

    def ahead_of(number, carry):
        for plane in range(CHUNK):
            for buffer in (pot, med):
                for tile in both:
                    for at in range(0, high, 8):
                        cell = (tile, number * CHUNK + plane + LEAD, slice(at, at + 8))
                        buffer[(1,) + cell] = roll(buffer[(0,) + cell], LANES - 1)
        return carry

    lax.fori_loop(0, planes // CHUNK, ahead_of, 0)

    def edges_of(z, carry):
        here = layer[z + 1] * 18
        there = {d: layer[z + 1 + d] * 18 for d in (-1, 0, 1)}
        own_g = [table[here + c] for c in range(9)]
        next_g = [table[there[o[0]] + c] for c, o in enumerate(OFFSETS)]
        flow_g = [table[here + 9 + c] + table[there[o[0]] + 9 + c] for c, o in enumerate(OFFSETS)]
        for tile in both:
            for block in range(inner + 2):
                at = 8 * block
                m = med[0, tile, z + LEAD, at : at + 8]
                v = pot[0, tile, z + LEAD, at : at + 8]
                inside = jnp.minimum(m, 1.0)
                tissue = jnp.maximum(m - 1.0, 0.0)
                bath = (inside - tissue) * (0.5 * bath_sigma)
                for column, (dz, dx, dy) in enumerate(OFFSETS):
                    if block == (0 if dx < 0 else inner + 1):
                        continue
                    row = at + dx
                    n = med[dy, tile, z + LEAD + dz, row : row + 8]
                    w = pot[dy, tile, z + LEAD + dz, row : row + 8]
                    n_in = jnp.minimum(n, 1.0)
                    n_ti = jnp.maximum(n - 1.0, 0.0)
                    mine = tissue * own_g[column]
                    other = n_ti * next_g[column]
                    if column < 3:
                        mine = mine + bath
                        other = other + (n_in - n_ti) * (0.5 * bath_sigma)
                    edge[column, tile, z + LEAD, at : at + 8] = n_in * mine + inside * other
                    vec[column, tile, z + LEAD, at : at + 8] = (
                        (tissue * n_ti) * flow_g[column]
                    ) * (w - v)
        return carry

    lax.fori_loop(0, planes, edges_of, 0)

    def lift(slot, side, z):
        for plane in range(CHUNK):
            for tile in both:
                for block in range(inner):
                    at = 8 + 8 * block
                    vec_l[side, tile, z + plane + LEAD, at : at + 8] = roll(
                        vec[slot, tile, z + plane + LEAD, at : at + 8], LANES - 1
                    )

    slot_of = lambda number: number - 1 if number else VECS

    def start_of(step, carry):
        base = step * CHUNK
        lift(slot_of(0), 0, base - CHUNK)
        for tile in both:
            for plane in range(CHUNK):
                z = base + plane
                for block in range(inner):
                    at = 8 + 8 * block
                    late_e, late_f = zero, zero
                    diagonal, flow = zero, zero
                    for column, (dz, dx, dy) in enumerate(OFFSETS):
                        back = (tile, z + LEAD - dz, slice(at - dx, at - dx + 8))
                        e = edge[(column,) + back]
                        f = vec[(column,) + back]
                        if dy:
                            late_e, late_f = late_e + e, late_f + f
                        else:
                            diagonal, flow = diagonal + e, flow - f
                        diagonal = diagonal + edge[column, tile, z + LEAD, at : at + 8]
                        flow = flow + vec[column, tile, z + LEAD, at : at + 8]
                    diagonal = diagonal + roll(late_e, 1)
                    flow = flow - roll(late_f, 1)
                    inside = jnp.minimum(med[0, tile, z + LEAD, at : at + 8], 1.0)
                    residual = flow + inside * (src[tile, z + LEAD, at : at + 8] - mean)
                    size = jnp.maximum(diagonal, 1.0)
                    scale = inside / size
                    jac[tile, z + LEAD, at : at + 8] = scale
                    kap[tile, z + LEAD, at : at + 8] = jnp.maximum(inside - diagonal, 0.0)
                    met[tile, z + LEAD, at : at + 8] = inside * size
                    vec[slot_of(0), tile, z + LEAD, at : at + 8] = scale * residual
        return carry

    lax.fori_loop(0, planes // CHUNK, start_of, 0)
    lift(slot_of(0), 0, planes - CHUNK)

    for step in range(ITERS):
        now, later, before = slot_of(step), slot_of(step + 1), slot_of(max(step - 1, 0))
        side, side_next = step % 2, (step + 1) % 2
        reach = ITERS - 1 - step
        low = jnp.maximum(first - reach, 0) // CHUNK
        up = (jnp.minimum(first + own_planes + reach, planes) + CHUNK - 1) // CHUNK

        def apply(number, carry):
            base = number * CHUNK
            if step + 1 < ITERS:
                lift(later, side_next, base - CHUNK)
            for tile in both:
                for block in range(inner) if step + 1 < ITERS else range(1, inner - 1):
                    at = 8 + 8 * block
                    for plane in range(CHUNK):
                        z = base + plane
                        total, late = zero, zero
                        for column, (dz, dx, dy) in enumerate(OFFSETS):
                            back = (tile, z + LEAD - dz, slice(at - dx, at - dx + 8))
                            product = edge[(column,) + back] * vec[(now,) + back]
                            if dy:
                                late = late + product
                            else:
                                total = total + product
                            ahead = (tile, z + LEAD + dz, slice(at + dx, at + dx + 8))
                            value = vec_l[(side,) + ahead] if dy else vec[(now,) + ahead]
                            total = total + edge[column, tile, z + LEAD, at : at + 8] * value
                        cell = (tile, z + LEAD, slice(at, at + 8))
                        total = total + kap[cell] * vec[(now,) + cell]
                        value = jac[cell] * (total + roll(late, 1))
                        if step:
                            value = 2.0 * value - vec[(before,) + cell]
                        vec[(later,) + cell] = value
            return carry

        lax.fori_loop(low, up, apply, 0)
        if step + 1 < ITERS:
            lift(later, side_next, (up - 1) * CHUNK)

    def joined(value):
        low = roll(value[0], LANES - SLOT)
        up = roll(value[1], SLOT)
        return jnp.where(lane < LANES // 2, low, up)

    def own_of(number, carry):
        for plane in range(CHUNK):
            z = number * CHUNK + plane
            for block in range(rows // 8):
                at = TOP + 8 * block
                out = 8 * block
                cell = lambda tile: (tile, first + z + LEAD, slice(at, at + 8))
                metric[z, out : out + 8] = joined([met[cell(tile)] for tile in both])
                for index in range(VECS):
                    basis[index, z, out : out + 8] = joined(
                        [vec[(slot_of(index),) + cell(tile)] for tile in both]
                    )
        return carry

    lax.fori_loop(0, own_planes // CHUNK, own_of, 0)

    pairs = [(i, j) for i in range(VECS) for j in range(i, VECS)]
    half = 26
    rowsum[...] = jnp.zeros(rowsum.shape, jnp.float32)
    for part, plain in ((pairs[:half], False), (pairs[half:], True)):

        def gather(z, carry):
            carry = list(carry)
            for block in range(rows // 8):
                out = 8 * block
                weight = metric[z, out : out + 8]
                used = range(VECS) if plain else sorted({k for pair in part for k in pair})
                loaded = {k: basis[k, z, out : out + 8] for k in used}
                scaled = {i: loaded[i] * weight for i in {i for i, _ in part} | ({0} if plain else set())}
                for number, (i, j) in enumerate(part):
                    carry[number] = carry[number] + scaled[i] * loaded[j]
                if plain:
                    for k in range(ITERS):
                        carry[len(part) + k] = carry[len(part) + k] + loaded[k]
                    carry[-1] = carry[-1] + scaled[0]
            return tuple(carry)

        count = len(part) + (ITERS + 1 if plain else 0)
        done = lax.fori_loop(0, own_planes, gather, tuple(zero for _ in range(count)))
        done = [jnp.sum(value, axis=0, keepdims=True) for value in done]
        for (i, j), value in zip(part, done):
            rowsum[VECS * i + j : VECS * i + j + 1] = value
            if i != j:
                rowsum[VECS * j + i : VECS * j + i + 1] = value
        for k, value in enumerate(done[len(part) :]):
            rowsum[SUMS + k : SUMS + k + 1] = value
    row = lax.dot_general(
        jnp.ones((8, LANES), jnp.float32),
        rowsum[...],
        (((1,), (1,)), ((), ())),
        precision=lax.Precision.HIGHEST,
        preferred_element_type=jnp.float32,
    )
    for at in range(0, gram.shape[0], 8):
        gram[at : at + 8] = row


def finish(geometry, gathered, total_in, basis, metric, solution_ref, residual_ref, flag):
    own_planes, rows = geometry
    total = jnp.sum(gathered[...], axis=0, keepdims=True)
    count = jnp.sum(total_in[0:1], axis=1, keepdims=True)
    lane = lane_iota((16, LANES))
    sub = lax.broadcasted_iota(jnp.int32, (16, LANES), 0)
    matrix = jnp.zeros((16, LANES), jnp.float32)
    for i in range(VECS):
        line = roll(total, LANES - VECS * i)
        matrix = jnp.where(sub == i, jnp.broadcast_to(line, (16, LANES)), matrix)
    matrix = jnp.where(lane < VECS, matrix, 0.0)
    reflected = jnp.where(lane == 0, roll(matrix, LANES - 1), roll(matrix, 1))
    square = matrix - 0.5 * (roll(matrix, LANES - 1) + reflected)
    system = jnp.where(lane < ITERS, square, 0.0)
    system = jnp.where(lane == ITERS, roll(matrix, ITERS), system)[0:8]
    lane8 = lane[0:8]
    sub8 = sub[0:8]
    for k in range(ITERS):
        line = system[k : k + 1]
        pivot = jnp.sum(jnp.where(lane8[0:1] == k, line, 0.0), axis=1, keepdims=True)
        line = line / pivot
        column = jnp.sum(jnp.where(lane8 == k, system, 0.0), axis=1, keepdims=True)
        line8 = jnp.broadcast_to(line, (8, LANES))
        system = jnp.where(sub8 == k, line8, system - column * line8)
    answer = jnp.sum(jnp.where(lane8 == ITERS, system, 0.0), axis=1, keepdims=True)
    coef = [answer[k : k + 1] for k in range(ITERS)]
    zero = jnp.zeros((1, 1), jnp.float32)
    padded = coef + [zero, zero]
    weights = []
    for i in range(VECS):
        value = 0.5 * padded[i + 1] - padded[i]
        if i == 0:
            value = value + 1.0
        elif i == 1:
            value = value + padded[0]
        else:
            value = value + 0.5 * padded[i - 1]
        weights.append(value)
    sums = [total[:, SUMS + k : SUMS + k + 1] for k in range(ITERS + 1)]
    mean = zero
    for k in range(ITERS):
        mean = mean + coef[k] * sums[k]
    mean = mean / count
    drift = sums[ITERS] / count
    column = jnp.concatenate(weights + [zero] * (16 - VECS), axis=0)
    row = jnp.zeros((1, LANES), jnp.float32)
    for i in range(VECS):
        row = jnp.where(lane[0:1] == i, weights[i], row)
    size = jnp.sum(jnp.sum(matrix * column * row, axis=1, keepdims=True), axis=0, keepdims=True)
    diagonal = jnp.sum(jnp.where(lane == sub, matrix, 0.0), axis=1, keepdims=True)
    spread = jnp.sum(jnp.abs(column) * jnp.sqrt(diagonal), axis=0, keepdims=True)
    flag[...] = jnp.broadcast_to(spread * spread / size, (8, LANES))

    def combine(z, carry):
        for block in range(rows // 8):
            out = 8 * block
            weight = metric[z, out : out + 8]
            inside = jnp.minimum(weight, 1.0)
            phi = inside * (-mean)
            rest = jnp.zeros((8, LANES), jnp.float32)
            for k in range(VECS):
                value = basis[k, z, out : out + 8]
                if k < ITERS:
                    phi = phi + coef[k] * value
                rest = rest + weights[k] * value
            solution_ref[z, out : out + 8] = phi
            residual_ref[z, out : out + 8] = weight * rest - inside * drift
        return carry

    lax.fori_loop(0, own_planes, combine, 0)


def f32(*shape):
    return jax.ShapeDtypeStruct(shape, jnp.float32)


def cyclic(count, shift):
    return [(i, (i + shift) % count) for i in range(count)]


def fast(potential, tissue_mask, layer_index, source):
    own_planes, rows, width = tissue_mask.shape
    gx, gy, gz = (lax.axis_size(name) for name in ("gx", "gy", "gz"))
    params = pltpu.CompilerParams(vmem_limit_bytes=60 * 1024 * 1024)
    stacked = jnp.stack([potential, source, tissue_mask.astype(jnp.float32)])

    full = gz * own_planes <= own_planes + 2 * HALO
    fields, layers = [stacked], [layer_index]
    if full:
        planes = gz * own_planes
        for shift in range(1, gz):
            fields.append(lax.ppermute(stacked, "gz", cyclic(gz, shift)))
            layers.append(lax.ppermute(layer_index, "gz", cyclic(gz, shift)))
    else:
        planes = own_planes + 2 * HALO
        left, hop = HALO, 1
        while left > 0:
            size = min(left, own_planes)
            up = [(i, i + hop) for i in range(gz - hop)]
            down = [(j, i) for i, j in up]
            fields.append(lax.ppermute(stacked[:, own_planes - size :], "gz", up))
            layers.append(lax.ppermute(layer_index[own_planes - size :], "gz", up))
            fields.append(lax.ppermute(stacked[:, :size], "gz", down))
            layers.append(lax.ppermute(layer_index[:size], "gz", down))
            left -= size
            hop += 1
    pieces = tuple(field.shape[1] for field in fields)
    summed = planes if full else own_planes
    groups = -(-planes // 8)
    y_rows = 3 * groups * rows + 8

    to_left, to_right, sums_own = pl.pallas_call(
        functools.partial(pack_y, (pieces, summed, rows)),
        out_shape=(f32(y_rows, LANES), f32(y_rows, LANES), f32(8, LANES)),
        in_specs=[VMEM] * len(pieces),
        out_specs=(VMEM,) * 3,
        compiler_params=params,
        name="pack_y",
    )(*fields)
    from_left = lax.ppermute(to_right, "gy", cyclic(gy, 1))
    from_right = lax.ppermute(to_left, "gy", cyclic(gy, gy - 1))
    last = 3 * groups * rows
    sums = sums_own + from_left[last:] + from_right[last:]
    for s in range(2, gy - 1):
        sums = sums + lax.ppermute(sums_own, "gy", cyclic(gy, s))
    extra = [lax.ppermute(sums, "gx", cyclic(gx, s)) for s in range(2, gx - 1)]
    extra.append(lax.ppermute(sums, "gx", [(0, gx - 1), (gx - 1, 0)]))

    strip = Strip(planes)
    upper, lower = pl.pallas_call(
        functools.partial(pack_x, (pieces, rows)),
        out_shape=(f32(strip.rows, LANES), f32(strip.rows, LANES)),
        in_specs=[VMEM] * (len(pieces) + 3),
        out_specs=(VMEM,) * 2,
        compiler_params=params,
        name="pack_x",
    )(*fields, from_left, from_right, sums)
    forth = [(i, i + 1) for i in range(gx - 1)]
    from_upper = lax.ppermute(lower, "gx", forth)
    from_lower = lax.ppermute(upper, "gx", [(j, i) for i, j in forth])
    if not full:
        sums = sums + from_upper[strip.sums :] + from_lower[strip.sums :] + sum(extra)
        sums = lax.psum(sums, "gz")
        extra = []

    table = np.concatenate(
        [
            0.5 * tensor_table(LAYERS, bulk_long, bulk_trans),
            0.5 * tensor_table(LAYERS, intra_long, intra_trans),
        ],
        axis=1,
    ).reshape(-1)
    high = TOP + rows + 16
    grid = (2, planes + LEAD + 1, high, LANES)
    everyone = gx * gy * gz
    gram, basis, metric, total = pl.pallas_call(
        functools.partial(krylov, (pieces, planes, own_planes, rows, len(extra), full, gz, gy)),
        out_shape=(
            f32(everyone, LANES),
            f32(VECS, own_planes, rows, LANES),
            f32(own_planes, rows, LANES),
            f32(8, LANES),
        ),
        in_specs=[SMEM] * (1 + len(pieces)) + [VMEM] * (len(pieces) + 5 + len(extra)),
        out_specs=(VMEM,) * 4,
        scratch_shapes=[
            pltpu.SMEM((planes + 2,), jnp.int32),
            pltpu.VMEM((2,) + grid, jnp.float32),
            pltpu.VMEM((2,) + grid, jnp.float32),
            pltpu.VMEM(grid, jnp.float32),
            pltpu.VMEM((len(OFFSETS),) + grid, jnp.float32),
            pltpu.VMEM((VECS + 1,) + grid, jnp.float32),
            pltpu.VMEM((2,) + grid, jnp.float32),
            pltpu.VMEM(grid, jnp.float32),
            pltpu.VMEM(grid, jnp.float32),
            pltpu.VMEM(grid, jnp.float32),
            pltpu.VMEM((LANES, LANES), jnp.float32),
        ],
        compiler_params=params,
        name="krylov",
    )(
        jnp.asarray(table),
        *layers,
        *fields,
        from_left,
        from_right,
        from_upper,
        from_lower,
        sums,
        *extra,
    )
    gathered = lax.all_to_all(gram, ("gx", "gy", "gz"), 0, 0, tiled=True)
    answer, residual, flag = pl.pallas_call(
        functools.partial(finish, (own_planes, rows)),
        out_shape=(f32(own_planes, rows, LANES), f32(own_planes, rows, LANES), f32(8, LANES)),
        in_specs=[VMEM] * 4,
        out_specs=(VMEM,) * 3,
        compiler_params=params,
        name="finish",
    )(gathered, total, basis, metric)
    return answer, residual, flag


def body(potential, tissue_mask, layer_index, source):
    answer, residual, flag = fast(potential, tissue_mask, layer_index, source)
    return (answer, residual)


def solution(mesh):
    placed = (P("gz", "gx", "gy"), P("gz", "gx", "gy"), P("gz"), P("gz", "gx", "gy"))
    return jax.shard_map(
        body,
        mesh=mesh,
        in_specs=placed,
        out_specs=(P("gz", "gx", "gy"), P("gz", "gx", "gy")),
        check_vma=False,
    )
```

```python
import functools
import math

import jax
import jax.numpy as jnp
import numpy as np
from jax import lax
from jax.experimental import pallas as pl
from jax.experimental.pallas import tpu as pltpu
from jax.sharding import PartitionSpec as P


ITERS = 8
LAYERS = 16
HALO = ITERS + 1
LANES = 128
SLOT = 16
TOP = 16
LEAD = 2
CHUNK = 2
VECS = ITERS + 1
LEAST_PIVOT = 0.02
SPREAD_LIMIT = 1e4
SUMS = VECS * VECS

OFFSETS = [
    (0, 1, 0),
    (0, 0, 1),
    (1, 0, 0),
    (0, 1, 1),
    (0, -1, 1),
    (1, 1, 0),
    (-1, 1, 0),
    (1, 0, 1),
    (-1, 0, 1),
]
STEPS = [(-dz, 1, -1) if (dz, dx, dy) == (0, -1, 1) else (dz, dx, dy) for dz, dx, dy in OFFSETS]
bulk_long = 7.99
bulk_trans = 2.55
intra_long = 1.74
intra_trans = 0.19
bath_sigma = 5.0

VMEM = pl.BlockSpec(memory_space=pltpu.VMEM)
SMEM = pl.BlockSpec(memory_space=pltpu.SMEM)


def tensor_table(layers, longitudinal, transverse):
    depth = np.arange(layers, dtype=np.float64) / (layers - 1)
    helix = math.pi / 3.0 * (1.0 - 2.0 * depth)
    tilted = 0.35 * np.cos(math.pi * depth)
    fiber_x = np.cos(tilted) * np.cos(helix)
    fiber_y = np.cos(tilted) * np.sin(helix)
    fiber_z = np.sin(tilted)
    spread = longitudinal - transverse
    s_xx = transverse + spread * fiber_x * fiber_x
    s_yy = transverse + spread * fiber_y * fiber_y
    s_zz = transverse + spread * fiber_z * fiber_z
    s_xy = spread * fiber_x * fiber_y
    s_xz = spread * fiber_x * fiber_z
    s_yz = spread * fiber_y * fiber_z
    columns = [
        s_xx - np.abs(s_xy) - np.abs(s_xz),
        s_yy - np.abs(s_xy) - np.abs(s_yz),
        s_zz - np.abs(s_xz) - np.abs(s_yz),
        np.maximum(s_xy, 0.0),
        np.maximum(-s_xy, 0.0),
        np.maximum(s_xz, 0.0),
        np.maximum(-s_xz, 0.0),
        np.maximum(s_yz, 0.0),
        np.maximum(-s_yz, 0.0),
    ]
    return np.stack(columns, axis=1).astype(np.float32)


def lane_iota(shape):
    return lax.broadcasted_iota(jnp.int32, shape, len(shape) - 1)


def roll(value, shift, axis=-1):
    axis = axis % value.ndim
    shift = shift % value.shape[axis]
    return value if shift == 0 else pltpu.roll(value, shift, axis)


def pack_y(geometry, *refs):
    pieces, summed, rows = geometry
    piece_refs = refs[: len(pieces)]
    left, right, sums = refs[len(pieces) :]
    listed = [(ref, plane) for ref, length in zip(piece_refs, pieces) for plane in range(length)]
    groups = -(-len(listed) // 8)
    lane = lane_iota((rows, LANES))
    count = jnp.zeros((rows, LANES), jnp.float32)
    total = jnp.zeros((rows, LANES), jnp.float32)
    for ref, plane in listed[:summed]:
        inside = jnp.minimum(ref[2, plane], 1.0)
        count = count + inside
        total = total + inside * ref[1, plane]
    sums[...] = jnp.zeros((8, LANES), jnp.float32)
    sums[0:1] = jnp.sum(count, axis=0, keepdims=True)
    sums[1:2] = jnp.sum(total, axis=0, keepdims=True)
    for field in range(3):
        for group in range(groups):
            to_left = jnp.zeros((rows, LANES), jnp.float32)
            to_right = jnp.zeros((rows, LANES), jnp.float32)
            for slot, (ref, plane) in enumerate(listed[8 * group : 8 * group + 8]):
                value = ref[field, plane]
                here = (lane >= SLOT * slot) & (lane < SLOT * (slot + 1))
                to_left = jnp.where(here, roll(value, SLOT * slot), to_left)
                to_right = jnp.where(here, roll(value, SLOT * (slot + 1)), to_right)
            base = (field * groups + group) * rows
            left[base : base + rows] = to_left
            right[base : base + rows] = to_right
    last = 3 * groups * rows
    left[last : last + 8] = sums[...]
    right[last : last + 8] = sums[...]


class Strip:
    def __init__(self, planes):
        self.planes = planes
        self.groups = -(-planes // 8)
        self.side = 3 * planes * 8
        self.ninth = self.side + 2 * 3 * self.groups * 8
        self.side_ninth = self.ninth + 2 * 8 * self.groups
        self.sums = self.side_ninth + -(-4 * self.groups // 8) * 8
        self.rows = self.sums + 8

    def own(self, field, plane):
        return (field * self.planes + plane) * 8

    def edge(self, side, field, group):
        return self.side + ((side * 3 + field) * self.groups + group) * 8

    def own_ninth(self, kind, group):
        return self.ninth + (kind * self.groups + group) * 8

    def edge_ninth(self, side, kind, group):
        return self.side_ninth + (side * 2 + kind) * self.groups + group


def pack_x(geometry, *refs):
    pieces, rows = geometry
    piece_refs = refs[: len(pieces)]
    from_left, from_right, total_ref, upper, lower = refs[len(pieces) :]
    listed = [(ref, plane) for ref, length in zip(piece_refs, pieces) for plane in range(length)]
    strip = Strip(len(listed))
    total = total_ref[...]
    for out, first, ninth in ((upper, 0, 8), (lower, rows - 8, rows - 9)):
        out[strip.ninth : strip.sums] = jnp.zeros((strip.sums - strip.ninth, LANES), jnp.float32)
        out[strip.sums : strip.rows] = total
        for number, (ref, plane) in enumerate(listed):
            for field in range(3):
                at = strip.own(field, number)
                out[at : at + 8] = ref[field, plane, first : first + 8]
            for kind, field in enumerate((0, 2)):
                at = strip.own_ninth(kind, number // 8) + number % 8
                out[at : at + 1] = ref[field, plane, ninth : ninth + 1]
        for side, packed in enumerate((from_left, from_right)):
            for group in range(strip.groups):
                for field in range(3):
                    at = strip.edge(side, field, group)
                    base = (field * strip.groups + group) * rows
                    out[at : at + 8] = packed[base + first : base + first + 8]
                for kind, field in enumerate((0, 2)):
                    at = strip.edge_ninth(side, kind, group)
                    base = (field * strip.groups + group) * rows
                    out[at : at + 1] = packed[base + ninth : base + ninth + 1]


def krylov(geometry, table, *refs):
    pieces, planes, own_planes, rows, extras, full, gz, gy = geometry
    layer_refs = refs[: len(pieces)]
    refs = refs[len(pieces) :]
    piece_refs = refs[: len(pieces)]
    refs = refs[len(pieces) :]
    from_left, from_right, from_upper, from_lower, own_sums = refs[:5]
    extra_refs = refs[5 : 5 + extras]
    refs = refs[5 + extras :]
    gram, basis, metric, total_out = refs[:4]
    layer, pot, med, src, edge, vec, vec_l, jac, kap, met, rowsum = refs[4:]
    high = TOP + rows + 16
    inner = (rows + 16) // 8
    both = (0, 1)
    strip = Strip(planes)
    groups = strip.groups
    lane = lane_iota((8, LANES))
    zero = jnp.zeros((8, LANES), jnp.float32)
    at_z = lax.axis_index("gz")
    at_y = lax.axis_index("gy")
    keep_left = jnp.where(at_y > 0, 1.0, 0.0)
    keep_right = jnp.where(at_y < gy - 1, 1.0, 0.0)

    if full:
        offsets = [lax.rem(at_z + gz - shift, gz) * own_planes for shift in range(gz)]
        first = offsets[0]
    else:
        offsets = [HALO]
        left = HALO
        for size in pieces[1::2]:
            offsets += [left - size, HALO + own_planes + HALO - left]
            left -= size
        first = HALO
    listed = [
        (ref, plane, offset + plane)
        for ref, length, offset in zip(piece_refs, pieces, offsets)
        for plane in range(length)
    ]
    layer[0] = 0
    layer[planes + 1] = 0
    for number, length in enumerate(pieces):
        for plane in range(length):
            layer[offsets[number] + plane + 1] = layer_refs[number][plane]

    totals = own_sums[...]
    if extras:
        totals = totals + from_upper[strip.sums : strip.rows] + from_lower[strip.sums : strip.rows]
    for ref in extra_refs:
        totals = totals + ref[...]
    total_out[...] = totals
    mean = jnp.sum(totals[1:2], axis=1, keepdims=True) / jnp.sum(
        totals[0:1], axis=1, keepdims=True
    )

    outside = (LEAD - 1, LEAD + planes)
    for plane in outside:
        for tile in both:
            for at in range(0, high, 8):
                for copy in both:
                    pot[copy, tile, plane, at : at + 8] = zero
                    med[copy, tile, plane, at : at + 8] = zero
                    vec_l[copy, tile, plane, at : at + 8] = zero
                for slot in range(VECS + 1):
                    vec[slot, tile, plane, at : at + 8] = zero
                for column, (dz, _, _) in enumerate(OFFSETS):
                    if dz:
                        edge[column, tile, plane, at : at + 8] = zero

    def tiles_of(own, strip_l, strip_r, slot, kind):
        ln = lane_iota(own.shape)
        a = roll(strip_l, LANES - SLOT * slot)
        b = roll(strip_r, LANES - SLOT * (slot + 1))
        if kind == 2:
            a, b = a * keep_left, b * keep_right
        low = jnp.where(ln < SLOT, a, roll(own, SLOT))
        up = jnp.where(ln >= LANES - SLOT, b, roll(own, LANES - SLOT))
        return low, up

    targets = {0: pot, 1: src, 2: med}

    def place(kind, tile, plane, at, value):
        size = value.shape[0]
        if kind == 1:
            src[tile, plane, at : at + size] = value
        else:
            targets[kind][0, tile, plane, at : at + size] = value

    for number, (ref, plane, z) in enumerate(listed):
        group, slot = divmod(number, 8)
        for field in range(3):
            base = (field * groups + group) * rows
            own = (
                ref[field, plane],
                from_left[base : base + rows],
                from_right[base : base + rows],
            )
            for tile, value in enumerate(tiles_of(*own, slot, field)):
                place(field, tile, z + LEAD, TOP, value)
            for packed, at in ((from_upper, TOP - 8), (from_lower, TOP + rows)):
                r0 = strip.own(field, number)
                r1 = strip.edge(0, field, group)
                r2 = strip.edge(1, field, group)
                halo = (packed[r0 : r0 + 8], packed[r1 : r1 + 8], packed[r2 : r2 + 8])
                for tile, value in enumerate(tiles_of(*halo, slot, field)):
                    place(field, tile, z + LEAD, at, value)
        for kind, field in enumerate((0, 2)):
            for packed, block, at in (
                (from_upper, 0, TOP - HALO),
                (from_lower, high - 8, TOP + rows + 8),
            ):
                r0 = strip.own_ninth(kind, group) + slot
                r1 = strip.edge_ninth(0, kind, group)
                r2 = strip.edge_ninth(1, kind, group)
                halo = (packed[r0 : r0 + 1], packed[r1 : r1 + 1], packed[r2 : r2 + 1])
                for tile, value in enumerate(tiles_of(*halo, slot, field)):
                    targets[field][0, tile, z + LEAD, block : block + 8] = zero
                    place(field, tile, z + LEAD, at, value)

    def ahead_of(number, carry):
        for plane in range(CHUNK):
            for buffer in (pot, med):
                for tile in both:
                    for at in range(0, high, 8):
                        cell = (tile, number * CHUNK + plane + LEAD, slice(at, at + 8))
                        buffer[(1,) + cell] = roll(buffer[(0,) + cell], LANES - 1)
        return carry

    lax.fori_loop(0, planes // CHUNK, ahead_of, 0)

    def edges_of(z, carry):
        here = layer[z + 1] * 18
        there = {d: layer[z + 1 + d] * 18 for d in (-1, 0, 1)}
        own_g = [table[here + c] for c in range(9)]
        next_g = [table[there[o[0]] + c] for c, o in enumerate(OFFSETS)]
        flow_g = [table[here + 9 + c] + table[there[o[0]] + 9 + c] for c, o in enumerate(OFFSETS)]
        for tile in both:
            for block in range(inner + 2):
                at = 8 * block
                m = med[0, tile, z + LEAD, at : at + 8]
                v = pot[0, tile, z + LEAD, at : at + 8]
                inside = jnp.minimum(m, 1.0)
                tissue = jnp.maximum(m - 1.0, 0.0)
                bath = (inside - tissue) * (0.5 * bath_sigma)
                for column, (dz, dx, dy) in enumerate(OFFSETS):
                    if block == (0 if dx < 0 else inner + 1):
                        continue
                    row = at + dx
                    n = med[dy, tile, z + LEAD + dz, row : row + 8]
                    w = pot[dy, tile, z + LEAD + dz, row : row + 8]
                    n_in = jnp.minimum(n, 1.0)
                    n_ti = jnp.maximum(n - 1.0, 0.0)
                    mine = tissue * own_g[column]
                    other = n_ti * next_g[column]
                    if column < 3:
                        mine = mine + bath
                        other = other + (n_in - n_ti) * (0.5 * bath_sigma)
                    edge[column, tile, z + LEAD, at : at + 8] = n_in * mine + inside * other
                    vec[column, tile, z + LEAD, at : at + 8] = (
                        (tissue * n_ti) * flow_g[column]
                    ) * (w - v)
        return carry

    lax.fori_loop(0, planes, edges_of, 0)

    def lift(slot, side, z):
        for plane in range(CHUNK):
            for tile in both:
                for block in range(inner):
                    at = 8 + 8 * block
                    vec_l[side, tile, z + plane + LEAD, at : at + 8] = roll(
                        vec[slot, tile, z + plane + LEAD, at : at + 8], LANES - 1
                    )

    slot_of = lambda number: number - 1 if number else VECS

    def start_of(step, carry):
        base = step * CHUNK
        lift(slot_of(0), 0, base - CHUNK)
        for tile in both:
            for plane in range(CHUNK):
                z = base + plane
                for block in range(inner):
                    at = 8 + 8 * block
                    late_e, late_f = zero, zero
                    diagonal, flow = zero, zero
                    for column, (dz, dx, dy) in enumerate(OFFSETS):
                        back = (tile, z + LEAD - dz, slice(at - dx, at - dx + 8))
                        e = edge[(column,) + back]
                        f = vec[(column,) + back]
                        if dy:
                            late_e, late_f = late_e + e, late_f + f
                        else:
                            diagonal, flow = diagonal + e, flow - f
                        diagonal = diagonal + edge[column, tile, z + LEAD, at : at + 8]
                        flow = flow + vec[column, tile, z + LEAD, at : at + 8]
                    diagonal = diagonal + roll(late_e, 1)
                    flow = flow - roll(late_f, 1)
                    inside = jnp.minimum(med[0, tile, z + LEAD, at : at + 8], 1.0)
                    residual = flow + inside * (src[tile, z + LEAD, at : at + 8] - mean)
                    size = jnp.maximum(diagonal, 1.0)
                    scale = inside / size
                    jac[tile, z + LEAD, at : at + 8] = scale
                    kap[tile, z + LEAD, at : at + 8] = jnp.maximum(inside - diagonal, 0.0)
                    met[tile, z + LEAD, at : at + 8] = inside * size
                    vec[slot_of(0), tile, z + LEAD, at : at + 8] = scale * residual
        return carry

    lax.fori_loop(0, planes // CHUNK, start_of, 0)
    lift(slot_of(0), 0, planes - CHUNK)

    for step in range(ITERS):
        now, later, before = slot_of(step), slot_of(step + 1), slot_of(max(step - 1, 0))
        side, side_next = step % 2, (step + 1) % 2
        reach = ITERS - 1 - step
        low = jnp.maximum(first - reach, 0) // CHUNK
        up = (jnp.minimum(first + own_planes + reach, planes) + CHUNK - 1) // CHUNK

        def apply(number, carry):
            base = number * CHUNK
            if step + 1 < ITERS:
                lift(later, side_next, base - CHUNK)
            for tile in both:
                for block in range(inner) if step + 1 < ITERS else range(1, inner - 1):
                    at = 8 + 8 * block
                    for plane in range(CHUNK):
                        z = base + plane
                        total, late = zero, zero
                        for column, (dz, dx, dy) in enumerate(OFFSETS):
                            back = (tile, z + LEAD - dz, slice(at - dx, at - dx + 8))
                            product = edge[(column,) + back] * vec[(now,) + back]
                            if dy:
                                late = late + product
                            else:
                                total = total + product
                            ahead = (tile, z + LEAD + dz, slice(at + dx, at + dx + 8))
                            value = vec_l[(side,) + ahead] if dy else vec[(now,) + ahead]
                            total = total + edge[column, tile, z + LEAD, at : at + 8] * value
                        cell = (tile, z + LEAD, slice(at, at + 8))
                        total = total + kap[cell] * vec[(now,) + cell]
                        value = jac[cell] * (total + roll(late, 1))
                        if step:
                            value = 2.0 * value - vec[(before,) + cell]
                        vec[(later,) + cell] = value
            return carry

        lax.fori_loop(low, up, apply, 0)
        if step + 1 < ITERS:
            lift(later, side_next, (up - 1) * CHUNK)

    def joined(value):
        low = roll(value[0], LANES - SLOT)
        up = roll(value[1], SLOT)
        return jnp.where(lane < LANES // 2, low, up)

    def own_of(number, carry):
        for plane in range(CHUNK):
            z = number * CHUNK + plane
            for block in range(rows // 8):
                at = TOP + 8 * block
                out = 8 * block
                cell = lambda tile: (tile, first + z + LEAD, slice(at, at + 8))
                metric[z, out : out + 8] = joined([met[cell(tile)] for tile in both])
                for index in range(VECS):
                    basis[index, z, out : out + 8] = joined(
                        [vec[(slot_of(index),) + cell(tile)] for tile in both]
                    )
        return carry

    lax.fori_loop(0, own_planes // CHUNK, own_of, 0)

    pairs = [(i, j) for i in range(VECS) for j in range(i, VECS)]
    half = 26
    rowsum[...] = jnp.zeros(rowsum.shape, jnp.float32)
    for part, plain in ((pairs[:half], False), (pairs[half:], True)):

        def gather(z, carry):
            carry = list(carry)
            for block in range(rows // 8):
                out = 8 * block
                weight = metric[z, out : out + 8]
                used = range(VECS) if plain else sorted({k for pair in part for k in pair})
                loaded = {k: basis[k, z, out : out + 8] for k in used}
                scaled = {i: loaded[i] * weight for i in {i for i, _ in part} | ({0} if plain else set())}
                for number, (i, j) in enumerate(part):
                    carry[number] = carry[number] + scaled[i] * loaded[j]
                if plain:
                    for k in range(ITERS):
                        carry[len(part) + k] = carry[len(part) + k] + loaded[k]
                    carry[-1] = carry[-1] + scaled[0]
            return tuple(carry)

        count = len(part) + (ITERS + 1 if plain else 0)
        done = lax.fori_loop(0, own_planes, gather, tuple(zero for _ in range(count)))
        done = [jnp.sum(value, axis=0, keepdims=True) for value in done]
        for (i, j), value in zip(part, done):
            rowsum[VECS * i + j : VECS * i + j + 1] = value
            if i != j:
                rowsum[VECS * j + i : VECS * j + i + 1] = value
        for k, value in enumerate(done[len(part) :]):
            rowsum[SUMS + k : SUMS + k + 1] = value
    row = lax.dot_general(
        jnp.ones((8, LANES), jnp.float32),
        rowsum[...],
        (((1,), (1,)), ((), ())),
        precision=lax.Precision.HIGHEST,
        preferred_element_type=jnp.float32,
    )
    for at in range(0, gram.shape[0], 8):
        gram[at : at + 8] = row


def finish(geometry, gathered, total_in, basis, metric, solution_ref, residual_ref, flag):
    own_planes, rows = geometry
    total = jnp.sum(gathered[...], axis=0, keepdims=True)
    count = jnp.sum(total_in[0:1], axis=1, keepdims=True)
    lane = lane_iota((8, LANES))
    sub = lax.broadcasted_iota(jnp.int32, (8, LANES), 0)
    pick = lambda index: jnp.sum(
        jnp.where(lane[0:1] == index, total, 0.0), axis=1, keepdims=True
    )
    last = pick(VECS * VECS - 1)
    sums = [pick(SUMS + k) for k in range(ITERS + 1)]
    matrix = jnp.zeros((8, LANES), jnp.float32)
    for i in range(ITERS):
        line = roll(total, LANES - VECS * i)
        matrix = jnp.where(sub == i, jnp.broadcast_to(line, (8, LANES)), matrix)
    columns = [
        jnp.broadcast_to(
            jnp.sum(jnp.where(lane == k, matrix, 0.0), axis=1, keepdims=True), (8, LANES)
        )
        for k in range(VECS)
    ]
    row_of = lambda value, k: jnp.broadcast_to(value[k : k + 1], (8, LANES))
    system = [columns[k] - 0.5 * (columns[k + 1] + columns[abs(k - 1)]) for k in range(ITERS)]
    diagonal = [row_of(system[k], k) for k in range(ITERS)]
    system.append(columns[0])
    least = jnp.ones((8, LANES), jnp.float32)
    for k in range(ITERS):
        pivot = row_of(system[k], k)
        least = jnp.minimum(least, pivot / diagonal[k])
        inverse = 1.0 / pivot
        for m in range(k + 1, ITERS + 1):
            line = row_of(system[m], k) * inverse
            system[m] = jnp.where(sub == k, line, system[m] - system[k] * line)
    answer = system[ITERS]
    coef = [row_of(answer, k) for k in range(ITERS)]
    after = jnp.where(sub == ITERS - 1, 0.0, roll(answer, 7, 0))
    before = jnp.where(sub == 0, 0.0, roll(answer, 1, 0))
    weight = 0.5 * (after + jnp.where(sub == 1, 2.0, 1.0) * before) - answer
    weight = jnp.where(sub == 0, weight + 1.0, weight)
    weights = [row_of(weight, k) for k in range(ITERS)] + [0.5 * coef[ITERS - 1]]
    mean = jnp.zeros((8, LANES), jnp.float32)
    for k in range(ITERS):
        mean = mean + coef[k] * sums[k]
    mean = mean / count
    drift = jnp.broadcast_to(sums[ITERS] / count, (8, LANES))

    product = jnp.zeros((8, LANES), jnp.float32)
    norms = jnp.zeros((8, LANES), jnp.float32)
    for k in range(VECS):
        product = product + weights[k] * columns[k]
        if k < ITERS:
            norms = jnp.where(sub == k, columns[k], norms)
    corner = jnp.sum(weight * columns[ITERS], axis=0, keepdims=True) + weights[ITERS] * last
    size = jnp.sum(weight * product, axis=0, keepdims=True) + weights[ITERS] * corner
    spread = jnp.sum(jnp.abs(weight) * jnp.sqrt(norms), axis=0, keepdims=True) + jnp.abs(
        weights[ITERS]
    ) * jnp.sqrt(last)
    fine = (least > LEAST_PIVOT) & (size > 0.0) & (spread * spread < SPREAD_LIMIT * size)
    flag[...] = jnp.where(fine, 1.0, 0.0)

    def combine(z, carry):
        for block in range(rows // 8):
            out = 8 * block
            scale = metric[z, out : out + 8]
            inside = jnp.minimum(scale, 1.0)
            phi = inside * (-mean)
            rest = jnp.zeros((8, LANES), jnp.float32)
            for k in range(VECS):
                value = basis[k, z, out : out + 8]
                if k < ITERS:
                    phi = phi + coef[k] * value
                rest = rest + weights[k] * value
            solution_ref[z, out : out + 8] = phi
            residual_ref[z, out : out + 8] = scale * rest - inside * drift
        return carry

    lax.fori_loop(0, own_planes, combine, 0)


def f32(*shape):
    return jax.ShapeDtypeStruct(shape, jnp.float32)


def cyclic(count, shift):
    return [(i, (i + shift) % count) for i in range(count)]


def fast(potential, tissue_mask, layer_index, source):
    own_planes, rows, _ = tissue_mask.shape
    gx, gy, gz = (lax.axis_size(name) for name in ("gx", "gy", "gz"))
    params = pltpu.CompilerParams(vmem_limit_bytes=60 * 1024 * 1024)
    stacked = jnp.stack([potential, source, tissue_mask.astype(jnp.float32)])

    full = gz * own_planes <= own_planes + 2 * HALO
    fields, layers = [stacked], [layer_index]
    if full:
        planes = gz * own_planes
        for shift in range(1, gz):
            fields.append(lax.ppermute(stacked, "gz", cyclic(gz, shift)))
            layers.append(lax.ppermute(layer_index, "gz", cyclic(gz, shift)))
    else:
        planes = own_planes + 2 * HALO
        left, hop = HALO, 1
        while left > 0:
            size = min(left, own_planes)
            up = [(i, i + hop) for i in range(gz - hop)]
            down = [(j, i) for i, j in up]
            fields.append(lax.ppermute(stacked[:, own_planes - size :], "gz", up))
            layers.append(lax.ppermute(layer_index[own_planes - size :], "gz", up))
            fields.append(lax.ppermute(stacked[:, :size], "gz", down))
            layers.append(lax.ppermute(layer_index[:size], "gz", down))
            left -= size
            hop += 1
    pieces = tuple(field.shape[1] for field in fields)
    summed = planes if full else own_planes
    groups = -(-planes // 8)
    y_rows = 3 * groups * rows + 8

    to_left, to_right, sums_own = pl.pallas_call(
        functools.partial(pack_y, (pieces, summed, rows)),
        out_shape=(f32(y_rows, LANES), f32(y_rows, LANES), f32(8, LANES)),
        in_specs=[VMEM] * len(pieces),
        out_specs=(VMEM,) * 3,
        compiler_params=params,
        name="pack_y",
    )(*fields)
    from_left = lax.ppermute(to_right, "gy", cyclic(gy, 1))
    from_right = lax.ppermute(to_left, "gy", cyclic(gy, gy - 1))
    last = 3 * groups * rows
    sums = sums_own + from_left[last:] + from_right[last:]
    for s in range(2, gy - 1):
        sums = sums + lax.ppermute(sums_own, "gy", cyclic(gy, s))
    far = [cyclic(gx, s) for s in range(2, gx - 1)] + [[(0, gx - 1), (gx - 1, 0)]]
    extra = []
    for pairs in far:
        extra.append(lax.ppermute(sums, "gx", pairs))

    strip = Strip(planes)
    upper, lower = pl.pallas_call(
        functools.partial(pack_x, (pieces, rows)),
        out_shape=(f32(strip.rows, LANES), f32(strip.rows, LANES)),
        in_specs=[VMEM] * (len(pieces) + 3),
        out_specs=(VMEM,) * 2,
        compiler_params=params,
        name="pack_x",
    )(*fields, from_left, from_right, sums)
    forth = [(i, i + 1) for i in range(gx - 1)]
    from_upper = lax.ppermute(lower, "gx", forth)
    from_lower = lax.ppermute(upper, "gx", [(j, i) for i, j in forth])
    if not full:
        sums = sums + from_upper[strip.sums :] + from_lower[strip.sums :] + sum(extra)
        sums = lax.psum(sums, "gz")
        extra = []

    table = np.concatenate(
        [
            0.5 * tensor_table(LAYERS, bulk_long, bulk_trans),
            0.5 * tensor_table(LAYERS, intra_long, intra_trans),
        ],
        axis=1,
    ).reshape(-1)
    high = TOP + rows + 16
    grid = (2, planes + LEAD + 1, high, LANES)
    everyone = gx * gy * gz
    gram, basis, metric, total = pl.pallas_call(
        functools.partial(krylov, (pieces, planes, own_planes, rows, len(extra), full, gz, gy)),
        out_shape=(
            f32(everyone, LANES),
            f32(VECS, own_planes, rows, LANES),
            f32(own_planes, rows, LANES),
            f32(8, LANES),
        ),
        in_specs=[SMEM] * (1 + len(pieces)) + [VMEM] * (len(pieces) + 5 + len(extra)),
        out_specs=(VMEM,) * 4,
        scratch_shapes=[
            pltpu.SMEM((planes + 2,), jnp.int32),
            pltpu.VMEM((2,) + grid, jnp.float32),
            pltpu.VMEM((2,) + grid, jnp.float32),
            pltpu.VMEM(grid, jnp.float32),
            pltpu.VMEM((len(OFFSETS),) + grid, jnp.float32),
            pltpu.VMEM((VECS + 1,) + grid, jnp.float32),
            pltpu.VMEM((2,) + grid, jnp.float32),
            pltpu.VMEM(grid, jnp.float32),
            pltpu.VMEM(grid, jnp.float32),
            pltpu.VMEM(grid, jnp.float32),
            pltpu.VMEM((LANES, LANES), jnp.float32),
        ],
        compiler_params=params,
        name="krylov",
    )(
        jnp.asarray(table),
        *layers,
        *fields,
        from_left,
        from_right,
        from_upper,
        from_lower,
        sums,
        *extra,
    )
    gathered = lax.all_to_all(gram, ("gx", "gy", "gz"), 0, 0, tiled=True)
    answer, residual, flag = pl.pallas_call(
        functools.partial(finish, (own_planes, rows)),
        out_shape=(f32(own_planes, rows, LANES), f32(own_planes, rows, LANES), f32(8, LANES)),
        in_specs=[VMEM] * 4,
        out_specs=(VMEM,) * 3,
        compiler_params=params,
        name="finish",
    )(gathered, total, basis, metric)
    return answer, residual, flag


def padded(value, sides, width):
    for axis, dim in sides:
        count, length = (lax.axis_size(axis), value.shape[dim])
        up = [(i, (i + 1) % count) for i in range(count - 1)]
        down = [(j, i) for i, j in up]
        last = lax.slice_in_dim(value, length - width, length, axis=dim)
        first = lax.slice_in_dim(value, 0, width, axis=dim)
        before = lax.ppermute(last, axis, up)
        after = lax.ppermute(first, axis, down)
        value = jnp.concatenate([before, value, after], axis=dim)
    return value


def window(array, offset, extent):
    return array[
        1 + offset[0] : 1 + offset[0] + extent[0],
        1 + offset[1] : 1 + offset[1] + extent[1],
        1 + offset[2] : 1 + offset[2] + extent[2],
    ]


def cell_weight(planes, column, tissue_pad, bath_pad):
    weight = tissue_pad * planes[:, column][:, None, None]
    if bath_pad is not None and column < 3:
        weight = weight + bath_sigma * bath_pad
    return weight


def edge_pair(weight, medium_pad, offset, extent):
    backward = (-offset[0], -offset[1], -offset[2])
    centre = window(medium_pad, (0, 0, 0), extent)
    own_weight = window(weight, (0, 0, 0), extent)
    forward_edge = (
        centre
        * window(medium_pad, offset, extent)
        * (0.5 * (own_weight + window(weight, offset, extent)))
    )
    backward_edge = (
        centre
        * window(medium_pad, backward, extent)
        * (0.5 * (own_weight + window(weight, backward, extent)))
    )
    return (forward_edge, backward_edge)


def with_rim(field):
    return padded(field, (("gx", 1), ("gy", 2), ("gz", 0)), 1)


def operate(field, edge_list):
    extent = field.shape
    field_pad = with_rim(field)
    summed = jnp.zeros(extent, jnp.float32)
    for column, offset in enumerate(STEPS):
        backward = (-offset[0], -offset[1], -offset[2])
        forward_edge, backward_edge = edge_list[column]
        summed = (
            summed
            + forward_edge * (field - window(field_pad, offset, extent))
            + backward_edge * (field - window(field_pad, backward, extent))
        )
    return summed


def plain(potential, tissue_mask, layer_index, source):
    extent = tissue_mask.shape
    mask_pad = padded(tissue_mask, (("gx", 1), ("gy", 2), ("gz", 0)), 1)
    layer_pad = padded(layer_index, (("gz", 0),), 1)
    selector = (layer_pad[:, None] == jnp.arange(LAYERS, dtype=jnp.int32)[None, :]).astype(
        jnp.float32
    )
    bulk_planes = jnp.dot(
        selector,
        jnp.asarray(tensor_table(LAYERS, bulk_long, bulk_trans)),
        precision=lax.Precision.HIGHEST,
    )
    intra_planes = jnp.dot(
        selector,
        jnp.asarray(tensor_table(LAYERS, intra_long, intra_trans)),
        precision=lax.Precision.HIGHEST,
    )
    tissue_pad = (mask_pad == 2).astype(jnp.float32)
    bath_pad = (mask_pad == 1).astype(jnp.float32)
    inside_pad = (mask_pad > 0).astype(jnp.float32)
    inside = window(inside_pad, (0, 0, 0), extent)
    bulk_edges = [
        edge_pair(
            cell_weight(bulk_planes, column, tissue_pad, bath_pad), inside_pad, offset, extent
        )
        for column, offset in enumerate(STEPS)
    ]
    intra_edges = [
        edge_pair(cell_weight(intra_planes, column, tissue_pad, None), tissue_pad, offset, extent)
        for column, offset in enumerate(STEPS)
    ]
    diagonal = jnp.zeros(extent, jnp.float32)
    for forward_edge, backward_edge in bulk_edges:
        diagonal = diagonal + forward_edge + backward_edge
    jacobi = inside / jnp.maximum(diagonal, 1.0)
    rhs = -operate(potential, intra_edges) + inside * source
    count, rhs_total = lax.psum((jnp.sum(inside), jnp.sum(rhs)), ("gx", "gy", "gz"))
    residual = rhs - inside * (rhs_total / count)
    solution = jnp.zeros(extent, jnp.float32)

    def coupled(current):
        scaled = jacobi * current
        image = operate(scaled, bulk_edges)
        scaled_total, cross_total, current_total, energy_total, image_total = lax.psum(
            (
                jnp.sum(scaled),
                jnp.sum(current * scaled),
                jnp.sum(current),
                jnp.sum(scaled * image),
                jnp.sum(image),
            ),
            ("gx", "gy", "gz"),
        )
        mean_value = scaled_total / count
        precond = scaled - inside * mean_value
        gamma_value = cross_total - mean_value * current_total
        delta_value = energy_total - mean_value * image_total
        return (precond, image, gamma_value, delta_value)

    def step(number, state):
        solution, residual, direction, along, gamma_now, alpha = state
        precond, image, gamma_next, delta = coupled(residual)
        begin = number == 0
        beta = jnp.where(begin, 0.0, gamma_next / jnp.where(begin, 1.0, gamma_now))
        scaled = jnp.where(begin, 0.0, beta * gamma_next / jnp.where(begin, 1.0, alpha))
        alpha = gamma_next / (delta - scaled)
        direction = precond + beta * direction
        along = image + beta * along
        solution = solution + alpha * direction
        residual = residual - alpha * along
        return (solution, residual, direction, along, gamma_next, alpha)

    empty = jnp.zeros(extent, jnp.float32)
    one = jnp.ones((), jnp.float32)
    state = (solution, residual, empty, empty, one, one)
    state = lax.fori_loop(0, ITERS, step, state)
    return state[:2]


def body(potential, tissue_mask, layer_index, source):
    args = (potential, tissue_mask, layer_index, source)
    answer, residual, flag = fast(*args)
    return lax.cond(
        flag[0, 0] > 0.5,
        lambda *_: (answer, residual),
        plain,
        *args,
    )


def solution(mesh):
    placed = (P("gz", "gx", "gy"), P("gz", "gx", "gy"), P("gz"), P("gz", "gx", "gy"))
    return jax.shard_map(
        body,
        mesh=mesh,
        in_specs=placed,
        out_specs=(P("gz", "gx", "gy"), P("gz", "gx", "gy")),
        check_vma=False,
    )
```

```python
import functools
import math

import jax
import jax.numpy as jnp
import numpy as np
from jax import lax
from jax.experimental import pallas as pl
from jax.experimental.pallas import tpu as pltpu
from jax.sharding import PartitionSpec as P


ITERS = 8
LAYERS = 16
SMALL_GRANT = 8 * 1024 * 1024
HALO = ITERS + 1
LANES = 128
SLOT = 16
TOP = 16
LEAD = 2
CHUNK = 2
VECS = ITERS + 1
LEAST_PIVOT = 0.02
SPREAD_LIMIT = 1e4
SUMS = VECS * VECS

OFFSETS = [
    (0, 1, 0),
    (0, 0, 1),
    (1, 0, 0),
    (0, 1, 1),
    (0, -1, 1),
    (1, 1, 0),
    (-1, 1, 0),
    (1, 0, 1),
    (-1, 0, 1),
]
STEPS = [(-dz, 1, -1) if (dz, dx, dy) == (0, -1, 1) else (dz, dx, dy) for dz, dx, dy in OFFSETS]
bulk_long = 7.99
bulk_trans = 2.55
intra_long = 1.74
intra_trans = 0.19
bath_sigma = 5.0

VMEM = pl.BlockSpec(memory_space=pltpu.VMEM)
SMEM = pl.BlockSpec(memory_space=pltpu.SMEM)


def tensor_table(layers, longitudinal, transverse):
    depth = np.arange(layers, dtype=np.float64) / (layers - 1)
    helix = math.pi / 3.0 * (1.0 - 2.0 * depth)
    tilted = 0.35 * np.cos(math.pi * depth)
    fiber_x = np.cos(tilted) * np.cos(helix)
    fiber_y = np.cos(tilted) * np.sin(helix)
    fiber_z = np.sin(tilted)
    spread = longitudinal - transverse
    s_xx = transverse + spread * fiber_x * fiber_x
    s_yy = transverse + spread * fiber_y * fiber_y
    s_zz = transverse + spread * fiber_z * fiber_z
    s_xy = spread * fiber_x * fiber_y
    s_xz = spread * fiber_x * fiber_z
    s_yz = spread * fiber_y * fiber_z
    columns = [
        s_xx - np.abs(s_xy) - np.abs(s_xz),
        s_yy - np.abs(s_xy) - np.abs(s_yz),
        s_zz - np.abs(s_xz) - np.abs(s_yz),
        np.maximum(s_xy, 0.0),
        np.maximum(-s_xy, 0.0),
        np.maximum(s_xz, 0.0),
        np.maximum(-s_xz, 0.0),
        np.maximum(s_yz, 0.0),
        np.maximum(-s_yz, 0.0),
    ]
    return np.stack(columns, axis=1).astype(np.float32)


def lane_iota(shape):
    return lax.broadcasted_iota(jnp.int32, shape, len(shape) - 1)


def roll(value, shift, axis=-1):
    axis = axis % value.ndim
    shift = shift % value.shape[axis]
    return value if shift == 0 else pltpu.roll(value, shift, axis)


def pack_y(geometry, *refs):
    pieces, summed, rows = geometry
    piece_refs = refs[: len(pieces)]
    left, right, sums = refs[len(pieces) :]
    listed = [(ref, plane) for ref, length in zip(piece_refs, pieces) for plane in range(length)]
    groups = -(-len(listed) // 8)
    lane = lane_iota((rows, LANES))
    count = jnp.zeros((rows, LANES), jnp.float32)
    total = jnp.zeros((rows, LANES), jnp.float32)
    for ref, plane in listed[:summed]:
        inside = jnp.minimum(ref[2, plane], 1.0)
        count = count + inside
        total = total + inside * ref[1, plane]
    sums[...] = jnp.zeros((8, LANES), jnp.float32)
    sums[0:1] = jnp.sum(count, axis=0, keepdims=True)
    sums[1:2] = jnp.sum(total, axis=0, keepdims=True)
    for field in range(3):
        for group in range(groups):
            to_left = jnp.zeros((rows, LANES), jnp.float32)
            to_right = jnp.zeros((rows, LANES), jnp.float32)
            for slot, (ref, plane) in enumerate(listed[8 * group : 8 * group + 8]):
                value = ref[field, plane]
                here = (lane >= SLOT * slot) & (lane < SLOT * (slot + 1))
                to_left = jnp.where(here, roll(value, SLOT * slot), to_left)
                to_right = jnp.where(here, roll(value, SLOT * (slot + 1)), to_right)
            base = (field * groups + group) * rows
            left[base : base + rows] = to_left
            right[base : base + rows] = to_right
    last = 3 * groups * rows
    left[last : last + 8] = sums[...]
    right[last : last + 8] = sums[...]


class Strip:
    def __init__(self, planes):
        self.planes = planes
        self.groups = -(-planes // 8)
        self.side = 3 * planes * 8
        self.ninth = self.side + 2 * 3 * self.groups * 8
        self.side_ninth = self.ninth + 2 * 8 * self.groups
        self.sums = self.side_ninth + -(-4 * self.groups // 8) * 8
        self.rows = self.sums + 8

    def own(self, field, plane):
        return (field * self.planes + plane) * 8

    def edge(self, side, field, group):
        return self.side + ((side * 3 + field) * self.groups + group) * 8

    def own_ninth(self, kind, group):
        return self.ninth + (kind * self.groups + group) * 8

    def edge_ninth(self, side, kind, group):
        return self.side_ninth + (side * 2 + kind) * self.groups + group


def pack_x(geometry, *refs):
    pieces, rows = geometry
    piece_refs = refs[: len(pieces)]
    from_left, from_right, total_ref, upper, lower = refs[len(pieces) :]
    listed = [(ref, plane) for ref, length in zip(piece_refs, pieces) for plane in range(length)]
    strip = Strip(len(listed))
    total = total_ref[...]
    for out, first, ninth in ((upper, 0, 8), (lower, rows - 8, rows - 9)):
        out[strip.ninth : strip.sums] = jnp.zeros((strip.sums - strip.ninth, LANES), jnp.float32)
        out[strip.sums : strip.rows] = total
        for number, (ref, plane) in enumerate(listed):
            for field in range(3):
                at = strip.own(field, number)
                out[at : at + 8] = ref[field, plane, first : first + 8]
            for kind, field in enumerate((0, 2)):
                at = strip.own_ninth(kind, number // 8) + number % 8
                out[at : at + 1] = ref[field, plane, ninth : ninth + 1]
        for side, packed in enumerate((from_left, from_right)):
            for group in range(strip.groups):
                for field in range(3):
                    at = strip.edge(side, field, group)
                    base = (field * strip.groups + group) * rows
                    out[at : at + 8] = packed[base + first : base + first + 8]
                for kind, field in enumerate((0, 2)):
                    at = strip.edge_ninth(side, kind, group)
                    base = (field * strip.groups + group) * rows
                    out[at : at + 1] = packed[base + ninth : base + ninth + 1]


def krylov(geometry, table, *refs):
    pieces, planes, own_planes, rows, extras, full, gz, gy = geometry
    layer_refs = refs[: len(pieces)]
    refs = refs[len(pieces) :]
    piece_refs = refs[: len(pieces)]
    refs = refs[len(pieces) :]
    from_left, from_right, from_upper, from_lower, own_sums = refs[:5]
    extra_refs = refs[5 : 5 + extras]
    refs = refs[5 + extras :]
    gram, basis, metric, total_out = refs[:4]
    layer, pot, med, src, edge, vec, vec_l, jac, kap, met, rowsum = refs[4:]
    high = TOP + rows + 16
    inner = (rows + 16) // 8
    both = (0, 1)
    strip = Strip(planes)
    groups = strip.groups
    lane = lane_iota((8, LANES))
    zero = jnp.zeros((8, LANES), jnp.float32)
    at_z = lax.axis_index("gz")
    at_y = lax.axis_index("gy")
    keep_left = jnp.where(at_y > 0, 1.0, 0.0)
    keep_right = jnp.where(at_y < gy - 1, 1.0, 0.0)

    if full:
        offsets = [lax.rem(at_z + gz - shift, gz) * own_planes for shift in range(gz)]
        first = offsets[0]
    else:
        offsets = [HALO]
        left = HALO
        for size in pieces[1::2]:
            offsets += [left - size, HALO + own_planes + HALO - left]
            left -= size
        first = HALO
    listed = [
        (ref, plane, offset + plane)
        for ref, length, offset in zip(piece_refs, pieces, offsets)
        for plane in range(length)
    ]
    layer[0] = 0
    layer[planes + 1] = 0
    for number, length in enumerate(pieces):
        for plane in range(length):
            layer[offsets[number] + plane + 1] = layer_refs[number][plane]

    totals = own_sums[...]
    if extras:
        totals = totals + from_upper[strip.sums : strip.rows] + from_lower[strip.sums : strip.rows]
    for ref in extra_refs:
        totals = totals + ref[...]
    total_out[...] = totals
    mean = jnp.sum(totals[1:2], axis=1, keepdims=True) / jnp.sum(
        totals[0:1], axis=1, keepdims=True
    )

    outside = (LEAD - 1, LEAD + planes)
    for plane in outside:
        for tile in both:
            for at in range(0, high, 8):
                for copy in both:
                    pot[copy, tile, plane, at : at + 8] = zero
                    med[copy, tile, plane, at : at + 8] = zero
                    vec_l[copy, tile, plane, at : at + 8] = zero
                for slot in range(VECS + 1):
                    vec[slot, tile, plane, at : at + 8] = zero
                for column, (dz, _, _) in enumerate(OFFSETS):
                    if dz:
                        edge[column, tile, plane, at : at + 8] = zero

    def tiles_of(own, strip_l, strip_r, slot, kind):
        ln = lane_iota(own.shape)
        a = roll(strip_l, LANES - SLOT * slot)
        b = roll(strip_r, LANES - SLOT * (slot + 1))
        if kind == 2:
            a, b = a * keep_left, b * keep_right
        low = jnp.where(ln < SLOT, a, roll(own, SLOT))
        up = jnp.where(ln >= LANES - SLOT, b, roll(own, LANES - SLOT))
        return low, up

    targets = {0: pot, 1: src, 2: med}

    def place(kind, tile, plane, at, value):
        size = value.shape[0]
        if kind == 1:
            src[tile, plane, at : at + size] = value
        else:
            targets[kind][0, tile, plane, at : at + size] = value

    for number, (ref, plane, z) in enumerate(listed):
        group, slot = divmod(number, 8)
        for field in range(3):
            base = (field * groups + group) * rows
            own = (
                ref[field, plane],
                from_left[base : base + rows],
                from_right[base : base + rows],
            )
            for tile, value in enumerate(tiles_of(*own, slot, field)):
                place(field, tile, z + LEAD, TOP, value)
            for packed, at in ((from_upper, TOP - 8), (from_lower, TOP + rows)):
                r0 = strip.own(field, number)
                r1 = strip.edge(0, field, group)
                r2 = strip.edge(1, field, group)
                halo = (packed[r0 : r0 + 8], packed[r1 : r1 + 8], packed[r2 : r2 + 8])
                for tile, value in enumerate(tiles_of(*halo, slot, field)):
                    place(field, tile, z + LEAD, at, value)
        for kind, field in enumerate((0, 2)):
            for packed, block, at in (
                (from_upper, 0, TOP - HALO),
                (from_lower, high - 8, TOP + rows + 8),
            ):
                r0 = strip.own_ninth(kind, group) + slot
                r1 = strip.edge_ninth(0, kind, group)
                r2 = strip.edge_ninth(1, kind, group)
                halo = (packed[r0 : r0 + 1], packed[r1 : r1 + 1], packed[r2 : r2 + 1])
                for tile, value in enumerate(tiles_of(*halo, slot, field)):
                    targets[field][0, tile, z + LEAD, block : block + 8] = zero
                    place(field, tile, z + LEAD, at, value)

    def ahead_of(number, carry):
        for plane in range(CHUNK):
            for buffer in (pot, med):
                for tile in both:
                    for at in range(0, high, 8):
                        cell = (tile, number * CHUNK + plane + LEAD, slice(at, at + 8))
                        buffer[(1,) + cell] = roll(buffer[(0,) + cell], LANES - 1)
        return carry

    lax.fori_loop(0, planes // CHUNK, ahead_of, 0)

    def edges_of(z, carry):
        here = layer[z + 1] * 18
        there = {d: layer[z + 1 + d] * 18 for d in (-1, 0, 1)}
        own_g = [table[here + c] for c in range(9)]
        next_g = [table[there[o[0]] + c] for c, o in enumerate(OFFSETS)]
        flow_g = [table[here + 9 + c] + table[there[o[0]] + 9 + c] for c, o in enumerate(OFFSETS)]
        for tile in both:
            for block in range(inner + 2):
                at = 8 * block
                m = med[0, tile, z + LEAD, at : at + 8]
                v = pot[0, tile, z + LEAD, at : at + 8]
                inside = jnp.minimum(m, 1.0)
                tissue = jnp.maximum(m - 1.0, 0.0)
                bath = (inside - tissue) * (0.5 * bath_sigma)
                for column, (dz, dx, dy) in enumerate(OFFSETS):
                    if block == (0 if dx < 0 else inner + 1):
                        continue
                    row = at + dx
                    n = med[dy, tile, z + LEAD + dz, row : row + 8]
                    w = pot[dy, tile, z + LEAD + dz, row : row + 8]
                    n_in = jnp.minimum(n, 1.0)
                    n_ti = jnp.maximum(n - 1.0, 0.0)
                    mine = tissue * own_g[column]
                    other = n_ti * next_g[column]
                    if column < 3:
                        mine = mine + bath
                        other = other + (n_in - n_ti) * (0.5 * bath_sigma)
                    edge[column, tile, z + LEAD, at : at + 8] = n_in * mine + inside * other
                    vec[column, tile, z + LEAD, at : at + 8] = (
                        (tissue * n_ti) * flow_g[column]
                    ) * (w - v)
        return carry

    lax.fori_loop(0, planes, edges_of, 0)

    def lift(slot, side, z):
        for plane in range(CHUNK):
            for tile in both:
                for block in range(inner):
                    at = 8 + 8 * block
                    vec_l[side, tile, z + plane + LEAD, at : at + 8] = roll(
                        vec[slot, tile, z + plane + LEAD, at : at + 8], LANES - 1
                    )

    slot_of = lambda number: number - 1 if number else VECS

    def start_of(step, carry):
        base = step * CHUNK
        lift(slot_of(0), 0, base - CHUNK)
        for tile in both:
            for plane in range(CHUNK):
                z = base + plane
                for block in range(inner):
                    at = 8 + 8 * block
                    late_e, late_f = zero, zero
                    diagonal, flow = zero, zero
                    for column, (dz, dx, dy) in enumerate(OFFSETS):
                        back = (tile, z + LEAD - dz, slice(at - dx, at - dx + 8))
                        e = edge[(column,) + back]
                        f = vec[(column,) + back]
                        if dy:
                            late_e, late_f = late_e + e, late_f + f
                        else:
                            diagonal, flow = diagonal + e, flow - f
                        diagonal = diagonal + edge[column, tile, z + LEAD, at : at + 8]
                        flow = flow + vec[column, tile, z + LEAD, at : at + 8]
                    diagonal = diagonal + roll(late_e, 1)
                    flow = flow - roll(late_f, 1)
                    inside = jnp.minimum(med[0, tile, z + LEAD, at : at + 8], 1.0)
                    residual = flow + inside * (src[tile, z + LEAD, at : at + 8] - mean)
                    size = jnp.maximum(diagonal, 1.0)
                    scale = inside / size
                    jac[tile, z + LEAD, at : at + 8] = scale
                    kap[tile, z + LEAD, at : at + 8] = jnp.maximum(inside - diagonal, 0.0)
                    met[tile, z + LEAD, at : at + 8] = inside * size
                    vec[slot_of(0), tile, z + LEAD, at : at + 8] = scale * residual
        return carry

    lax.fori_loop(0, planes // CHUNK, start_of, 0)
    lift(slot_of(0), 0, planes - CHUNK)

    for step in range(ITERS):
        now, later, before = slot_of(step), slot_of(step + 1), slot_of(max(step - 1, 0))
        side, side_next = step % 2, (step + 1) % 2
        reach = ITERS - 1 - step
        low = jnp.maximum(first - reach, 0) // CHUNK
        up = (jnp.minimum(first + own_planes + reach, planes) + CHUNK - 1) // CHUNK

        def apply(number, carry):
            base = number * CHUNK
            if step + 1 < ITERS:
                lift(later, side_next, base - CHUNK)
            for tile in both:
                for block in range(inner) if step + 1 < ITERS else range(1, inner - 1):
                    at = 8 + 8 * block
                    for plane in range(CHUNK):
                        z = base + plane
                        total, late = zero, zero
                        for column, (dz, dx, dy) in enumerate(OFFSETS):
                            back = (tile, z + LEAD - dz, slice(at - dx, at - dx + 8))
                            product = edge[(column,) + back] * vec[(now,) + back]
                            if dy:
                                late = late + product
                            else:
                                total = total + product
                            ahead = (tile, z + LEAD + dz, slice(at + dx, at + dx + 8))
                            value = vec_l[(side,) + ahead] if dy else vec[(now,) + ahead]
                            total = total + edge[column, tile, z + LEAD, at : at + 8] * value
                        cell = (tile, z + LEAD, slice(at, at + 8))
                        total = total + kap[cell] * vec[(now,) + cell]
                        value = jac[cell] * (total + roll(late, 1))
                        if step:
                            value = 2.0 * value - vec[(before,) + cell]
                        vec[(later,) + cell] = value
            return carry

        lax.fori_loop(low, up, apply, 0)
        if step + 1 < ITERS:
            lift(later, side_next, (up - 1) * CHUNK)

    def joined(value):
        low = roll(value[0], LANES - SLOT)
        up = roll(value[1], SLOT)
        return jnp.where(lane < LANES // 2, low, up)

    def own_of(number, carry):
        for plane in range(CHUNK):
            z = number * CHUNK + plane
            for block in range(rows // 8):
                at = TOP + 8 * block
                out = 8 * block
                cell = lambda tile: (tile, first + z + LEAD, slice(at, at + 8))
                metric[z, out : out + 8] = joined([met[cell(tile)] for tile in both])
                for index in range(VECS):
                    basis[index, z, out : out + 8] = joined(
                        [vec[(slot_of(index),) + cell(tile)] for tile in both]
                    )
        return carry

    lax.fori_loop(0, own_planes // CHUNK, own_of, 0)

    pairs = [(i, j) for i in range(VECS) for j in range(i, VECS)]
    half = 26
    rowsum[...] = jnp.zeros(rowsum.shape, jnp.float32)
    for part, plain in ((pairs[:half], False), (pairs[half:], True)):

        def gather(z, carry):
            carry = list(carry)
            for block in range(rows // 8):
                out = 8 * block
                weight = metric[z, out : out + 8]
                used = range(VECS) if plain else sorted({k for pair in part for k in pair})
                loaded = {k: basis[k, z, out : out + 8] for k in used}
                scaled = {i: loaded[i] * weight for i in {i for i, _ in part} | ({0} if plain else set())}
                for number, (i, j) in enumerate(part):
                    carry[number] = carry[number] + scaled[i] * loaded[j]
                if plain:
                    for k in range(ITERS):
                        carry[len(part) + k] = carry[len(part) + k] + loaded[k]
                    carry[-1] = carry[-1] + scaled[0]
            return tuple(carry)

        count = len(part) + (ITERS + 1 if plain else 0)
        done = lax.fori_loop(0, own_planes, gather, tuple(zero for _ in range(count)))
        done = [jnp.sum(value, axis=0, keepdims=True) for value in done]
        for (i, j), value in zip(part, done):
            rowsum[VECS * i + j : VECS * i + j + 1] = value
            if i != j:
                rowsum[VECS * j + i : VECS * j + i + 1] = value
        for k, value in enumerate(done[len(part) :]):
            rowsum[SUMS + k : SUMS + k + 1] = value
    row = lax.dot_general(
        jnp.ones((8, LANES), jnp.float32),
        rowsum[...],
        (((1,), (1,)), ((), ())),
        precision=lax.Precision.HIGHEST,
        preferred_element_type=jnp.float32,
    )
    for at in range(0, gram.shape[0], 8):
        gram[at : at + 8] = row


def finish(geometry, gathered, total_in, basis, metric, solution_ref, residual_ref, flag):
    own_planes, rows = geometry
    total = jnp.sum(gathered[...], axis=0, keepdims=True)
    count = jnp.sum(total_in[0:1], axis=1, keepdims=True)
    lane = lane_iota((8, LANES))
    sub = lax.broadcasted_iota(jnp.int32, (8, LANES), 0)
    pick = lambda index: jnp.sum(
        jnp.where(lane[0:1] == index, total, 0.0), axis=1, keepdims=True
    )
    last = pick(VECS * VECS - 1)
    sums = [pick(SUMS + k) for k in range(ITERS + 1)]
    matrix = jnp.zeros((8, LANES), jnp.float32)
    for i in range(ITERS):
        line = roll(total, LANES - VECS * i)
        matrix = jnp.where(sub == i, jnp.broadcast_to(line, (8, LANES)), matrix)
    columns = [
        jnp.broadcast_to(
            jnp.sum(jnp.where(lane == k, matrix, 0.0), axis=1, keepdims=True), (8, LANES)
        )
        for k in range(VECS)
    ]
    row_of = lambda value, k: jnp.broadcast_to(value[k : k + 1], (8, LANES))
    system = [columns[k] - 0.5 * (columns[k + 1] + columns[abs(k - 1)]) for k in range(ITERS)]
    diagonal = [row_of(system[k], k) for k in range(ITERS)]
    system.append(columns[0])
    least = jnp.ones((8, LANES), jnp.float32)
    for k in range(ITERS):
        pivot = row_of(system[k], k)
        least = jnp.minimum(least, pivot / diagonal[k])
        inverse = 1.0 / pivot
        for m in range(k + 1, ITERS + 1):
            line = row_of(system[m], k) * inverse
            system[m] = jnp.where(sub == k, line, system[m] - system[k] * line)
    answer = system[ITERS]
    coef = [row_of(answer, k) for k in range(ITERS)]
    after = jnp.where(sub == ITERS - 1, 0.0, roll(answer, 7, 0))
    before = jnp.where(sub == 0, 0.0, roll(answer, 1, 0))
    weight = 0.5 * (after + jnp.where(sub == 1, 2.0, 1.0) * before) - answer
    weight = jnp.where(sub == 0, weight + 1.0, weight)
    weights = [row_of(weight, k) for k in range(ITERS)] + [0.5 * coef[ITERS - 1]]
    mean = jnp.zeros((8, LANES), jnp.float32)
    for k in range(ITERS):
        mean = mean + coef[k] * sums[k]
    mean = mean / count
    drift = jnp.broadcast_to(sums[ITERS] / count, (8, LANES))

    product = jnp.zeros((8, LANES), jnp.float32)
    norms = jnp.zeros((8, LANES), jnp.float32)
    for k in range(VECS):
        product = product + weights[k] * columns[k]
        if k < ITERS:
            norms = jnp.where(sub == k, columns[k], norms)
    corner = jnp.sum(weight * columns[ITERS], axis=0, keepdims=True) + weights[ITERS] * last
    size = jnp.sum(weight * product, axis=0, keepdims=True) + weights[ITERS] * corner
    spread = jnp.sum(jnp.abs(weight) * jnp.sqrt(norms), axis=0, keepdims=True) + jnp.abs(
        weights[ITERS]
    ) * jnp.sqrt(last)
    fine = (least > LEAST_PIVOT) & (size > 0.0) & (spread * spread < SPREAD_LIMIT * size)
    flag[0] = jnp.max(jnp.where(fine, 1.0, 0.0)).astype(jnp.int32)

    def combine(z, carry):
        for block in range(rows // 8):
            out = 8 * block
            scale = metric[z, out : out + 8]
            inside = jnp.minimum(scale, 1.0)
            phi = inside * (-mean)
            rest = jnp.zeros((8, LANES), jnp.float32)
            for k in range(VECS):
                value = basis[k, z, out : out + 8]
                if k < ITERS:
                    phi = phi + coef[k] * value
                rest = rest + weights[k] * value
            solution_ref[z, out : out + 8] = phi
            residual_ref[z, out : out + 8] = scale * rest - inside * drift
        return carry

    lax.fori_loop(0, own_planes, combine, 0)


def f32(*shape):
    return jax.ShapeDtypeStruct(shape, jnp.float32)


def cyclic(count, shift):
    return [(i, (i + shift) % count) for i in range(count)]


def fast(potential, tissue_mask, layer_index, source):
    own_planes, rows, _ = tissue_mask.shape
    gx, gy, gz = (lax.axis_size(name) for name in ("gx", "gy", "gz"))
    params = pltpu.CompilerParams(vmem_limit_bytes=SMALL_GRANT)
    stacked = jnp.stack([potential, source, tissue_mask.astype(jnp.float32)])

    full = gz * own_planes <= own_planes + 2 * HALO
    fields, layers = [stacked], [layer_index]
    if full:
        planes = gz * own_planes
        for shift in range(1, gz):
            layers.append(lax.ppermute(layer_index, "gz", cyclic(gz, shift)))
            fields.append(lax.ppermute(stacked, "gz", cyclic(gz, shift)))
    else:
        planes = own_planes + 2 * HALO
        left, hop = HALO, 1
        while left > 0:
            size = min(left, own_planes)
            up = [(i, i + hop) for i in range(gz - hop)]
            down = [(j, i) for i, j in up]
            fields.append(lax.ppermute(stacked[:, own_planes - size :], "gz", up))
            layers.append(lax.ppermute(layer_index[own_planes - size :], "gz", up))
            fields.append(lax.ppermute(stacked[:, :size], "gz", down))
            layers.append(lax.ppermute(layer_index[:size], "gz", down))
            left -= size
            hop += 1
    pieces = tuple(field.shape[1] for field in fields)
    summed = planes if full else own_planes
    groups = -(-planes // 8)
    y_rows = 3 * groups * rows + 8

    to_left, to_right, sums_own = pl.pallas_call(
        functools.partial(pack_y, (pieces, summed, rows)),
        out_shape=(f32(y_rows, LANES), f32(y_rows, LANES), f32(8, LANES)),
        in_specs=[VMEM] * len(pieces),
        out_specs=(VMEM,) * 3,
        compiler_params=params,
        name="pack_y",
    )(*fields)
    from_left = lax.ppermute(to_right, "gy", cyclic(gy, 1))
    from_right = lax.ppermute(to_left, "gy", cyclic(gy, gy - 1))
    last = 3 * groups * rows
    sums = sums_own + from_left[last:] + from_right[last:]
    for s in range(2, gy - 1):
        from_far = lax.ppermute(sums_own, "gy", cyclic(gy, s))
        sums = sums + from_far
    far = [cyclic(gx, s) for s in range(2, gx - 1)] + [[(0, gx - 1), (gx - 1, 0)]]
    extra = []
    if full and len(far) == gz == 2:
        pairs = [(i * gz + core, j * gz + core) for core in range(gz) for i, j in far[core]]
        extra.append(lax.ppermute(sums, ("gx", "gz"), pairs))
        extra.append(lax.ppermute(extra[0], "gz", cyclic(gz, 1)))
    else:
        for pairs in far:
            extra.append(lax.ppermute(sums, "gx", pairs))

    strip = Strip(planes)
    upper, lower = pl.pallas_call(
        functools.partial(pack_x, (pieces, rows)),
        out_shape=(f32(strip.rows, LANES), f32(strip.rows, LANES)),
        in_specs=[VMEM] * (len(pieces) + 3),
        out_specs=(VMEM,) * 2,
        compiler_params=params,
        name="pack_x",
    )(*fields, from_left, from_right, sums)
    forth = [(i, i + 1) for i in range(gx - 1)]
    from_upper = lax.ppermute(lower, "gx", forth)
    from_lower = lax.ppermute(upper, "gx", [(j, i) for i, j in forth])
    if not full:
        sums = sums + from_upper[strip.sums :] + from_lower[strip.sums :] + sum(extra)
        sums = lax.psum(sums, "gz")
        extra = []

    table = np.concatenate(
        [
            0.5 * tensor_table(LAYERS, bulk_long, bulk_trans),
            0.5 * tensor_table(LAYERS, intra_long, intra_trans),
        ],
        axis=1,
    ).reshape(-1)
    high = TOP + rows + 16
    grid = (2, planes + LEAD + 1, high, LANES)
    scratch = [
        (2,) + grid,
        (2,) + grid,
        grid,
        (len(OFFSETS),) + grid,
        (VECS + 1,) + grid,
        (2,) + grid,
        grid,
        grid,
        grid,
        (LANES, LANES),
    ]
    everyone = gx * gy * gz
    gram, basis, metric, total = pl.pallas_call(
        functools.partial(krylov, (pieces, planes, own_planes, rows, len(extra), full, gz, gy)),
        out_shape=(
            f32(everyone, LANES),
            f32(VECS, own_planes, rows, LANES),
            f32(own_planes, rows, LANES),
            f32(8, LANES),
        ),
        in_specs=[SMEM] * (1 + len(pieces)) + [VMEM] * (len(pieces) + 5 + len(extra)),
        out_specs=(VMEM,) * 4,
        scratch_shapes=[
            pltpu.SMEM((planes + 2,), jnp.int32),
            *[pltpu.VMEM(shape, jnp.float32) for shape in scratch],
        ],
        compiler_params=pltpu.CompilerParams(
            vmem_limit_bytes=SMALL_GRANT + 4 * sum(math.prod(shape) for shape in scratch)
        ),
        name="krylov",
    )(
        jnp.asarray(table),
        *layers,
        *fields,
        from_left,
        from_right,
        from_upper,
        from_lower,
        sums,
        *extra,
    )
    gathered = lax.all_to_all(gram, ("gx", "gy", "gz"), 0, 0, tiled=True)
    answer, residual, flag = pl.pallas_call(
        functools.partial(finish, (own_planes, rows)),
        out_shape=(
            f32(own_planes, rows, LANES),
            f32(own_planes, rows, LANES),
            jax.ShapeDtypeStruct((1,), jnp.int32),
        ),
        in_specs=[VMEM] * 4,
        out_specs=(VMEM, VMEM, SMEM),
        compiler_params=params,
        name="finish",
    )(gathered, total, basis, metric)
    return answer, residual, flag


def padded(value, sides, width):
    for axis, dim in sides:
        count, length = (lax.axis_size(axis), value.shape[dim])
        up = [(i, (i + 1) % count) for i in range(count - 1)]
        down = [(j, i) for i, j in up]
        last = lax.slice_in_dim(value, length - width, length, axis=dim)
        first = lax.slice_in_dim(value, 0, width, axis=dim)
        before = lax.ppermute(last, axis, up)
        after = lax.ppermute(first, axis, down)
        value = jnp.concatenate([before, value, after], axis=dim)
    return value


def window(array, offset, extent):
    return array[
        1 + offset[0] : 1 + offset[0] + extent[0],
        1 + offset[1] : 1 + offset[1] + extent[1],
        1 + offset[2] : 1 + offset[2] + extent[2],
    ]


def cell_weight(planes, column, tissue_pad, bath_pad):
    weight = tissue_pad * planes[:, column][:, None, None]
    if bath_pad is not None and column < 3:
        weight = weight + bath_sigma * bath_pad
    return weight


def edge_pair(weight, medium_pad, offset, extent):
    backward = (-offset[0], -offset[1], -offset[2])
    centre = window(medium_pad, (0, 0, 0), extent)
    own_weight = window(weight, (0, 0, 0), extent)
    forward_edge = (
        centre
        * window(medium_pad, offset, extent)
        * (0.5 * (own_weight + window(weight, offset, extent)))
    )
    backward_edge = (
        centre
        * window(medium_pad, backward, extent)
        * (0.5 * (own_weight + window(weight, backward, extent)))
    )
    return (forward_edge, backward_edge)


def with_rim(field):
    return padded(field, (("gx", 1), ("gy", 2), ("gz", 0)), 1)


def operate(field, edge_list):
    extent = field.shape
    field_pad = with_rim(field)
    summed = jnp.zeros(extent, jnp.float32)
    for column, offset in enumerate(STEPS):
        backward = (-offset[0], -offset[1], -offset[2])
        forward_edge, backward_edge = edge_list[column]
        summed = (
            summed
            + forward_edge * (field - window(field_pad, offset, extent))
            + backward_edge * (field - window(field_pad, backward, extent))
        )
    return summed


def plain(potential, tissue_mask, layer_index, source):
    extent = tissue_mask.shape
    mask_pad = padded(tissue_mask, (("gx", 1), ("gy", 2), ("gz", 0)), 1)
    layer_pad = padded(layer_index, (("gz", 0),), 1)
    selector = (layer_pad[:, None] == jnp.arange(LAYERS, dtype=jnp.int32)[None, :]).astype(
        jnp.float32
    )
    bulk_planes = jnp.dot(
        selector,
        jnp.asarray(tensor_table(LAYERS, bulk_long, bulk_trans)),
        precision=lax.Precision.HIGHEST,
    )
    intra_planes = jnp.dot(
        selector,
        jnp.asarray(tensor_table(LAYERS, intra_long, intra_trans)),
        precision=lax.Precision.HIGHEST,
    )
    tissue_pad = (mask_pad == 2).astype(jnp.float32)
    bath_pad = (mask_pad == 1).astype(jnp.float32)
    inside_pad = (mask_pad > 0).astype(jnp.float32)
    inside = window(inside_pad, (0, 0, 0), extent)
    bulk_edges = [
        edge_pair(
            cell_weight(bulk_planes, column, tissue_pad, bath_pad), inside_pad, offset, extent
        )
        for column, offset in enumerate(STEPS)
    ]
    intra_edges = [
        edge_pair(cell_weight(intra_planes, column, tissue_pad, None), tissue_pad, offset, extent)
        for column, offset in enumerate(STEPS)
    ]
    diagonal = jnp.zeros(extent, jnp.float32)
    for forward_edge, backward_edge in bulk_edges:
        diagonal = diagonal + forward_edge + backward_edge
    jacobi = inside / jnp.maximum(diagonal, 1.0)
    rhs = -operate(potential, intra_edges) + inside * source
    count, rhs_total = lax.psum((jnp.sum(inside), jnp.sum(rhs)), ("gx", "gy", "gz"))
    residual = rhs - inside * (rhs_total / count)
    solution = jnp.zeros(extent, jnp.float32)

    def coupled(current):
        scaled = jacobi * current
        image = operate(scaled, bulk_edges)
        scaled_total, cross_total, current_total, energy_total, image_total = lax.psum(
            (
                jnp.sum(scaled),
                jnp.sum(current * scaled),
                jnp.sum(current),
                jnp.sum(scaled * image),
                jnp.sum(image),
            ),
            ("gx", "gy", "gz"),
        )
        mean_value = scaled_total / count
        precond = scaled - inside * mean_value
        gamma_value = cross_total - mean_value * current_total
        delta_value = energy_total - mean_value * image_total
        return (precond, image, gamma_value, delta_value)

    def step(number, state):
        solution, residual, direction, along, gamma_now, alpha = state
        precond, image, gamma_next, delta = coupled(residual)
        begin = number == 0
        beta = jnp.where(begin, 0.0, gamma_next / jnp.where(begin, 1.0, gamma_now))
        scaled = jnp.where(begin, 0.0, beta * gamma_next / jnp.where(begin, 1.0, alpha))
        alpha = gamma_next / (delta - scaled)
        direction = precond + beta * direction
        along = image + beta * along
        solution = solution + alpha * direction
        residual = residual - alpha * along
        return (solution, residual, direction, along, gamma_next, alpha)

    empty = jnp.zeros(extent, jnp.float32)
    one = jnp.ones((), jnp.float32)
    state = (solution, residual, empty, empty, one, one)
    state = lax.fori_loop(0, ITERS, step, state)
    return state[:2]


def body(potential, tissue_mask, layer_index, source):
    args = (potential, tissue_mask, layer_index, source)
    answer, residual, flag = fast(*args)
    return lax.cond(
        flag[0] > 0,
        lambda *_: (answer, residual),
        plain,
        *args,
    )


def solution(mesh):
    placed = (P("gz", "gx", "gy"), P("gz", "gx", "gy"), P("gz"), P("gz", "gx", "gy"))
    return jax.shard_map(
        body,
        mesh=mesh,
        in_specs=placed,
        out_specs=(P("gz", "gx", "gy"), P("gz", "gx", "gy")),
        check_vma=False,
    )
```
